128 devices in a mesh: rows: 128 (over y, z, x, core).
Axes of the slice: x: 4, y: 4, z: 4, core: 2. Of those that a mesh axis runs over, the one named last changes fastest.
Arguments:
- source: bfloat16 [262144, 128], P('rows'), may hold values from -6 to 6
- target: bfloat16 [262144, 128], P('rows'), may hold values from -6 to 6
- tile_values: bfloat16 [16384, 128, 128], P('rows'), may hold values from -0.25 to 0.25
- tile_rows: int32 [16384], P('rows'), may hold values from 0 to 15
- tile_peers: int32 [16384], P('rows'), may hold values from 0 to 127
- need_list: int32 [128, 128], P('rows'), may hold values from 0 to 15
- tile_count: int32 [128], P('rows'), may hold values from 1 to 128, as said below
Outputs:
- source_embed: bfloat16 [262144, 128], P('rows')
- target_embed: bfloat16 [262144, 128], P('rows')
The draws below stay inside these ranges and needn't reach their ends.
Inputs may be any that keep to these rules, and one draw needn't show every extreme that they name: `tile_count`: some device has 128 live tiles; tiles in slots at or past the count take no part.
All inputs are finite; a program needn't handle non-finite values.
Results may differ from the reference program's by a relative error of at most 0.0053.
Values may be sent and summed in bfloat16 or wider, within the bound.
No kernel may reach another device: no remote copies, remote signals or barrier semaphores. Data moves between devices by JAX's collectives and lax.ppermute only.
A program may use at most 128 MiB of HBM per device.

```python
import math
import jax
import jax.numpy as jnp
import numpy as np
from jax import lax

W = 128
BLOCK = 128
RB = 16
TILES_DEV = 128
ITERS = 2
NODES = 262144
DEVICES = 128


def draw_tile_count(key, part):
    ranks = jax.random.permutation(key, DEVICES)
    counts = TILES_DEV * 16 // (16 + ranks)
    return jnp.maximum(counts, 1).astype(jnp.int32)


def plant(values, rng, least, high):
    longest = values.shape.index(max(values.shape))
    spots = []
    for shift in (0, 1):
        where = [jax.random.randint(jax.random.fold_in(rng, axis), (), 0, length) for axis, length in enumerate(values.shape)]
        where[longest] = (where[longest] + shift) % values.shape[longest]
        spots.append(tuple(where))
    return values.at[spots[0]].set(least).at[spots[1]].set(high)


def levels(stream_key, extent, split, smallest, top_value):
    level, own = 1.0, jax.random.fold_in(stream_key, 6)
    for axis_at, shards_of in split:
        draws = jnp.exp(jax.random.uniform(jax.random.fold_in(own, axis_at), (shards_of,), jnp.float32, smallest / len(split), top_value / len(split)))
        level = level * jnp.repeat(draws, extent[axis_at] // shards_of).reshape([-1 if axis == axis_at else 1 for axis in range(len(extent))])
    return level


def cumulative_ranks(amount, skew):
    portions = [(1 << 20) // math.isqrt(grade ** skew) + 1 for grade in range(1, amount + 1)]
    width = 1 + sum(portions) // (1 << 30)
    return np.cumsum(np.array([max(1, weight // width) for weight in portions]))


def ranked(own_key, shape, count, lean):
    grid = cumulative_ranks(count, lean)
    pick = jax.random.randint(jax.random.fold_in(own_key, 1), shape, 0, int(grid[count - 1]))
    grade = jnp.searchsorted(jnp.asarray(grid, jnp.int32), pick, side="right")
    return jax.random.permutation(jax.random.fold_in(own_key, 2), count)[grade].astype(jnp.int32)


def bell_draw(stream_key, shape, deviation, most, cuts=(), kind=jnp.bfloat16):
    values = deviation * jax.random.normal(stream_key, shape, jnp.float32)
    if cuts:
        values = values * levels(stream_key, shape, cuts, -0.22, 0.18)
    return jnp.clip(values, -most, most).astype(kind)


def setup_inputs(seed: int = 0) -> dict:
    arg_keys = jax.random.split(jax.random.key(seed), 8)
    source = bell_draw(arg_keys[0], (NODES, W), 1.0, 6.0, ((0, 128),))
    target = bell_draw(arg_keys[1], (NODES, W), 1.0, 6.0, ((0, 128),))
    tile_values = bell_draw(arg_keys[2], (DEVICES * TILES_DEV, BLOCK, BLOCK), (BLOCK * 4) ** -0.5, 0.25, ((0, 128),))
    tile_rows = plant(jax.random.randint(arg_keys[3], (DEVICES * TILES_DEV,), 0, RB), jax.random.fold_in(arg_keys[3], 1), 0, RB - 1).astype(jnp.int32)
    tile_peers = plant(ranked(arg_keys[4], (DEVICES * TILES_DEV,), DEVICES, 2), jax.random.fold_in(arg_keys[4], 3), 0, DEVICES - 1).astype(jnp.int32)
    need_list = plant(jax.random.randint(arg_keys[5], (DEVICES, DEVICES), 0, RB), jax.random.fold_in(arg_keys[5], 1), 0, RB - 1).astype(jnp.int32)
    tile_count = draw_tile_count(jax.random.fold_in(arg_keys[7], 71), 0)
    return {"source": source, "target": target, "tile_values": tile_values, "tile_rows": tile_rows, "tile_peers": tile_peers, "need_list": need_list, "tile_count": tile_count}


epsilon = 1e-06

def settle(base, update):
    total = base.astype(jnp.float32) + update
    scale = lax.rsqrt(lax.optimization_barrier(jnp.mean(total * total, axis=-1, keepdims=True)) + epsilon)
    return (total * scale).astype(jnp.bfloat16)

def reference(source, target, tile_values, tile_rows, tile_peers, need_list, tile_count):
    tile_side = tile_values.shape[1]
    feature_width = source.shape[1]
    tiles = tile_values.reshape(DEVICES, TILES_DEV, tile_side, tile_side)
    row_ids = tile_rows.reshape(DEVICES, TILES_DEV).astype(jnp.int32)
    peer_ids = tile_peers.reshape(DEVICES, TILES_DEV).astype(jnp.int32)
    device_ids = jnp.arange(DEVICES, dtype=jnp.int32)[:, None]
    row_blocks = device_ids * RB + row_ids
    col_blocks = peer_ids * RB + jnp.take_along_axis(need_list.astype(jnp.int32), peer_ids, axis=1)
    live_mask = (jnp.arange(TILES_DEV, dtype=jnp.int32)[None, :] < tile_count[:, None]).astype(jnp.float32)
    source_now, target_now = (source, target)
    for iteration in range(ITERS):
        source_blocks = source_now.reshape(-1, tile_side, feature_width).astype(jnp.float32)
        target_blocks = target_now.reshape(-1, tile_side, feature_width).astype(jnp.float32)

        def one_device(target_sum, device):
            tile_block = tiles[device].astype(jnp.float32)
            alive = live_mask[device][:, None, None]
            forward = jnp.einsum('tij,tjk->tik', tile_block, source_blocks[col_blocks[device]], precision=lax.Precision.HIGHEST) * alive
            gathered = jax.ops.segment_sum(forward, row_ids[device], num_segments=RB)
            backward = jnp.einsum('tji,tjk->tik', tile_block, target_blocks[row_blocks[device]], precision=lax.Precision.HIGHEST) * alive
            target_sum = target_sum.at[col_blocks[device]].add(backward)
            return (target_sum, gathered)
        start_sum = jnp.zeros((DEVICES * RB, tile_side, feature_width), jnp.float32)
        target_sum, gathered = lax.scan(one_device, start_sum, jnp.arange(DEVICES, dtype=jnp.int32))
        source_now = settle(source, gathered.reshape(-1, feature_width))
        target_now = settle(target, target_sum.reshape(-1, feature_width))
    return (source_now, target_now)
```

```python
import functools
import jax
import jax.numpy as jnp
from jax import lax
from jax.experimental import pallas as pl
from jax.experimental.pallas import tpu as pltpu
from jax.sharding import PartitionSpec as P

ITERS = 2
epsilon = 1e-06

SIDE = 128
OWN = 16
CAP = 63
PITCH = OWN + CAP + 1
META = PITCH - 1
F32 = jnp.float32
BF16 = jnp.bfloat16
MIB = 1 << 20


def settle(base, update):
    total = base.astype(F32) + update
    scale = lax.rsqrt(jnp.mean(total * total, axis=-1, keepdims=True) + epsilon)
    return (total * scale).astype(BF16)


def block(ref, index):
    return ref[pl.ds(pl.multiple_of(index * SIDE, SIDE), SIDE), :]


def pack_rows(scr, x_ref, acc, peers, buf):
    for b in range(OWN):
        scr[pl.ds(b, SIDE, stride=PITCH), :] = x_ref[b * SIDE : (b + 1) * SIDE, :].astype(F32)

    def put(c, _):
        scr[pl.ds(OWN + c, SIDE, stride=PITCH), :] = block(acc, c)
        return 0

    lax.fori_loop(0, peers, put, 0)

    def narrow(i, _):
        buf[i] = scr[pl.ds(pl.multiple_of(i * PITCH, 8), PITCH), :].astype(BF16)
        return 0

    lax.fori_loop(0, SIDE, narrow, 0, unroll=4)


def zero(ref, blocks):
    def one(c, _):
        ref[pl.ds(pl.multiple_of(c * SIDE, SIDE), SIDE), :] = jnp.zeros((SIDE, SIDE), F32)
        return 0

    lax.fori_loop(0, blocks, one, 0)


def back_dot(tile, y):
    return lax.dot_general(tile, y, (((0,), (0,)), ((), ())), preferred_element_type=F32)


STEP = 4


def first_kernel(
    count, rows, peers_ref, need_ref, tiles, x_ref, y_ref, buf, slots, scr, acc, slot_v, sem
):
    live = count[0]
    row_at = lax.broadcasted_iota(jnp.int32, (SIDE, SIDE), 0)
    lane_at = lax.broadcasted_iota(jnp.int32, (SIDE, SIDE), 1)
    hit = jnp.where((row_at == peers_ref[...]) & (lane_at < live), 1.0, 0.0)
    used = jnp.broadcast_to(jnp.max(hit, axis=1, keepdims=True), (SIDE, SIDE))
    below = jnp.where(lane_at < row_at, 1.0, 0.0).astype(BF16)
    slot = jnp.dot(below, used.astype(BF16), preferred_element_type=F32)
    total = jnp.sum(used, axis=0, keepdims=True)
    lane = lax.broadcasted_iota(jnp.int32, (1, SIDE), 1)
    mine = jnp.sum(hit * slot, axis=0, keepdims=True)
    mine = jnp.where(lane < live, jnp.minimum(mine, float(CAP)), float(CAP))
    peer_total = jnp.minimum(total, float(CAP))
    slot_v[0:1, :] = mine.astype(jnp.int32)
    slot_v[1:2, :] = peer_total.astype(jnp.int32)
    copy = pltpu.make_async_copy(slot_v, slots, sem)
    copy.start()
    at = jnp.where(used > 0, slot, -1.0)
    pick = at == lane_at.astype(F32)
    peer_of = jnp.sum(jnp.where(pick, row_at.astype(F32), 0.0), axis=0, keepdims=True)
    peer_of = jnp.where(lane.astype(F32) < total, peer_of, float(SIDE))
    need_col = jnp.sum(
        jnp.where(row_at == lane_at, need_ref[...], 0).astype(F32), axis=1, keepdims=True
    )
    pick = (at == (lane_at - CAP - 1).astype(F32)) & (lane_at > CAP)
    need_of = jnp.sum(jnp.where(pick, need_col, 0.0), axis=0, keepdims=True)
    meta = jnp.where(lane < CAP, peer_of, jnp.where(lane == CAP, total, need_of))
    scr[pl.ds(META, SIDE, stride=PITCH), :] = jnp.broadcast_to(meta, (SIDE, SIDE))
    copy.wait()
    peers = slots[1, 0]
    zero(acc, peers)

    def step(g, _):
        parts = []
        for k in range(STEP):
            t = g * STEP + k
            parts.append((slots[0, t], back_dot(tiles[t], block(y_ref, rows[t]))))
        for s, part in parts:
            where = pl.ds(pl.multiple_of(s * SIDE, SIDE), SIDE)
            acc[where, :] = acc[where, :] + part
        return 0

    lax.fori_loop(0, (live + STEP - 1) // STEP, step, 0)
    pack_rows(scr, x_ref, acc, peers, buf)


LANES8 = 8


def middle_kernel(index, counts, recv, buf, xs, acc, parts, outs):
    def load(d, _):
        at = pl.ds(pl.multiple_of(d * OWN, OWN), OWN)
        xs[at, :] = recv[d, 0:OWN, :].astype(F32)
        acc[at, :] = jnp.zeros((OWN, SIDE), F32)
        return 0

    lax.fori_loop(0, SIDE, load, 0, unroll=4)
    xs[OWN * SIDE :, :] = jnp.zeros((8, SIDE), F32)

    def reader(d, _):
        def batch(b, _):
            start = pl.multiple_of(b * LANES8, LANES8)
            parts[pl.ds(start, LANES8), :] = recv[d, pl.ds(OWN + start, LANES8), :].astype(F32)
            spots = [index[d, start + k] for k in range(LANES8)]
            sums = []
            for k, spot in enumerate(spots):
                outs[pl.ds(d * (CAP + 1) + start + k, 1), :] = xs[pl.ds(spot, 1), :]
                sums.append(acc[pl.ds(spot, 1), :] + parts[pl.ds(start + k, 1), :])
            for k, spot in enumerate(spots):
                acc[pl.ds(spot, 1), :] = sums[k]
            return 0

        lax.fori_loop(0, (counts[d] + LANES8 - 1) // LANES8, batch, 0)
        return 0

    lax.fori_loop(0, SIDE, reader, 0)

    def narrow(d, _):
        buf[d, 0:OWN, :] = acc[pl.ds(pl.multiple_of(d * OWN, OWN), OWN), :].astype(BF16)
        at = pl.ds(pl.multiple_of(d * (CAP + 1), CAP + 1), CAP + 1)
        buf[d, OWN:PITCH, :] = outs[at, :].astype(BF16)
        return 0

    lax.fori_loop(0, SIDE, narrow, 0, unroll=4)


def tail_kernel(
    last, count, rows, slots, recv, tiles, source, target, *rest
):
    if last:
        x_new, y_new, scr, xb, acc_x = rest
        buf = acc = None
    else:
        buf, scr, xb, acc_x, acc, x_new, y_new = rest
    live = count[0]
    peers = slots[1, 0]

    def widen(i, _):
        scr[pl.ds(pl.multiple_of(i * PITCH, 8), PITCH), :] = recv[i].astype(F32)
        return 0

    lax.fori_loop(0, SIDE, widen, 0, unroll=4)
    for b in range(OWN):
        at = slice(b * SIDE, (b + 1) * SIDE)
        y_new[at, :] = settle(target[at, :], scr[pl.ds(b, SIDE, stride=PITCH), :])

    def fetch(c, _):
        xb[pl.ds(pl.multiple_of(c * SIDE, SIDE), SIDE), :] = scr[
            pl.ds(OWN + c, SIDE, stride=PITCH), :
        ].astype(BF16)
        return 0

    lax.fori_loop(0, peers, fetch, 0)
    zero(acc_x, OWN)
    if not last:
        zero(acc, peers)

    def step(g, _):
        ahead, back = [], []
        for k in range(STEP):
            t = g * STEP + k
            s, r, tile = slots[0, t], rows[t], tiles[t]
            to = jnp.where(t < live, r, OWN)
            ahead.append((to, jnp.dot(tile, block(xb, s), preferred_element_type=F32)))
            if not last:
                back.append((s, back_dot(tile, block(y_new, r))))
        for ref, found in ((acc_x, ahead), (acc, back)):
            for s, part in found:
                where = pl.ds(pl.multiple_of(s * SIDE, SIDE), SIDE)
                ref[where, :] = ref[where, :] + part
        return 0

    lax.fori_loop(0, (live + STEP - 1) // STEP, step, 0)
    for b in range(OWN):
        at = slice(b * SIDE, (b + 1) * SIDE)
        x_new[at, :] = settle(source[at, :], acc_x[at, :])
    if not last:
        pack_rows(scr, x_new, acc, peers, buf)


def vmem(shape, dtype):
    return pltpu.VMEM(shape, dtype)


IN_VMEM = pl.BlockSpec(memory_space=pltpu.VMEM)
IN_SMEM = pl.BlockSpec(memory_space=pltpu.SMEM)
BUF = jax.ShapeDtypeStruct((SIDE, PITCH, SIDE), BF16)
NODES = jax.ShapeDtypeStruct((OWN * SIDE, SIDE), BF16)


def fast(source, target, tile_values, tile_rows, tile_peers, need_list, tile_count):
    swap = lambda value: lax.all_to_all(value, "rows", split_axis=0, concat_axis=0, tiled=True)
    buf, slots = pl.pallas_call(
        first_kernel,
        out_shape=(BUF, jax.ShapeDtypeStruct((8, SIDE), jnp.int32)),
        in_specs=[IN_SMEM] * 2 + [IN_VMEM] * 5,
        out_specs=(IN_VMEM, IN_SMEM),
        scratch_shapes=[
            vmem((SIDE * PITCH, SIDE), F32),
            vmem(((CAP + 1) * SIDE, SIDE), F32),
            vmem((8, SIDE), jnp.int32),
            pltpu.SemaphoreType.DMA,
        ],
        compiler_params=pltpu.CompilerParams(vmem_limit_bytes=28 * MIB),
        name="first",
    )(
        tile_count,
        tile_rows,
        tile_peers.reshape(1, SIDE),
        need_list.reshape(1, SIDE),
        tile_values,
        source,
        target,
    )
    recv = swap(buf)
    meta = recv[:, META, :].astype(F32)
    counts = meta[:, CAP].astype(jnp.int32)
    spots = (meta[:, :CAP] * OWN + meta[:, CAP + 1 : 2 * CAP + 1]).astype(jnp.int32)
    index = jnp.pad(spots, ((0, 0), (0, 1)), constant_values=OWN * SIDE)
    carried = jnp.minimum(counts, CAP)
    middle = pl.pallas_call(
        middle_kernel,
        out_shape=BUF,
        in_specs=[IN_SMEM] * 2 + [IN_VMEM],
        out_specs=IN_VMEM,
        scratch_shapes=[
            vmem((OWN * SIDE + 8, SIDE), F32),
            vmem((OWN * SIDE + 8, SIDE), F32),
            vmem((CAP + 1, SIDE), F32),
            vmem((SIDE * (CAP + 1), SIDE), F32),
        ],
        compiler_params=pltpu.CompilerParams(vmem_limit_bytes=28 * MIB),
        name="middle",
    )
    for iteration in range(ITERS):
        recv = swap(middle(index, carried, recv))
        last = iteration == ITERS - 1
        wide = vmem((SIDE * PITCH, SIDE), F32)
        xb = vmem(((CAP + 1) * SIDE, SIDE), BF16)
        acc_x = vmem(((OWN + 1) * SIDE, SIDE), F32)
        acc = vmem(((CAP + 1) * SIDE, SIDE), F32)
        node = vmem((OWN * SIDE, SIDE), BF16)
        out = pl.pallas_call(
            functools.partial(tail_kernel, last),
            out_shape=(NODES, NODES) if last else BUF,
            in_specs=[IN_SMEM] * 3 + [IN_VMEM] * 4,
            out_specs=(IN_VMEM, IN_VMEM) if last else IN_VMEM,
            scratch_shapes=[wide, xb, acc_x] if last else [wide, xb, acc_x, acc, node, node],
            compiler_params=pltpu.CompilerParams(vmem_limit_bytes=32 * MIB),
            name="last" if last else "tail",
        )(tile_count, tile_rows, slots, recv, tile_values, source, target)
        if not last:
            recv = swap(out)
    return out, jnp.max(counts) > CAP


def general(source, target, tile_values, tile_rows, tile_peers, need_list, tile_count):
    peers_total = lax.axis_size("rows")
    row_count = source.shape[0] // SIDE
    tiles_here = tile_values.shape[0]
    group = min(16, tiles_here)
    live = (jnp.arange(tiles_here, dtype=jnp.int32) < tile_count[0]).astype(F32)[:, None, None]
    swap = lambda value: lax.all_to_all(value, "rows", split_axis=0, concat_axis=0, tiled=True)
    send_list = swap(need_list.reshape(peers_total, 1))[:, 0]
    owner_hot = (send_list[None, :] == jnp.arange(row_count, dtype=jnp.int32)[:, None]).astype(F32)

    def take(value, position):
        return lax.dynamic_slice_in_dim(value, position * group, group, 0)

    def product(form, vectors, position, ids):
        return (
            jnp.einsum(form, take(tile_values, position), vectors[ids], preferred_element_type=F32)
            * take(live, position)
        )

    def iterate(_, state):
        source_now, target_now = state
        source_blocks = source_now.reshape(row_count, SIDE, SIDE)
        target_blocks = target_now.reshape(row_count, SIDE, SIDE)

        def backward(position, running):
            part = product("tji,tjk->tik", target_blocks, position, take(tile_rows, position))
            return running.at[take(tile_peers, position)].add(part)

        partial = lax.fori_loop(
            0, tiles_here // group, backward, jnp.zeros((peers_total, SIDE, SIDE), F32)
        )
        both = swap(jnp.stack([source_blocks[send_list], partial.astype(BF16)], axis=1))
        fetched = both[:, 0]

        def forward(position, running):
            part = product("tij,tjk->tik", fetched, position, take(tile_peers, position))
            return running.at[take(tile_rows, position)].add(part)

        gathered = lax.fori_loop(
            0, tiles_here // group, forward, jnp.zeros((row_count, SIDE, SIDE), F32)
        )
        incoming = jnp.dot(
            owner_hot,
            both[:, 1].astype(F32).reshape(peers_total, -1),
            precision=lax.Precision.HIGHEST,
            preferred_element_type=F32,
        )
        return (
            settle(source, gathered.reshape(-1, SIDE)),
            settle(target, incoming.reshape(-1, SIDE)),
        )

    return lax.fori_loop(0, ITERS, iterate, (source, target))


def shards(*args):
    found, over = fast(*args)
    return lax.cond(over, lambda: general(*args), lambda: found)


def solution(mesh):
    return jax.shard_map(
        shards,
        mesh=mesh,
        in_specs=(
            P("rows", None),
            P("rows", None),
            P("rows", None, None),
            P("rows"),
            P("rows"),
            P("rows", None),
            P("rows"),
        ),
        out_specs=(P("rows", None), P("rows", None)),
        check_vma=False,
    )
```

```python
import functools
import jax
import jax.numpy as jnp
from jax import lax
from jax.experimental import pallas as pl
from jax.experimental.pallas import tpu as pltpu
from jax.sharding import PartitionSpec as P

ITERS = 2
epsilon = 1e-06

SIDE = 128
OWN = 16
CAP = 63
PITCH = OWN + CAP + 1
META = PITCH - 1
STRIDE = PITCH + 1
F32 = jnp.float32
BF16 = jnp.bfloat16
MIB = 1 << 20


def settle(base, update):
    total = base.astype(F32) + update
    scale = lax.rsqrt(jnp.mean(total * total, axis=-1, keepdims=True) + epsilon)
    return (total * scale).astype(BF16)


def block(ref, index):
    return ref[pl.ds(pl.multiple_of(index * SIDE, SIDE), SIDE), :]


def pack_rows(scr, x_ref, acc, peers, buf):
    for b in range(OWN):
        scr[pl.ds(b, SIDE, stride=STRIDE), :] = x_ref[b * SIDE : (b + 1) * SIDE, :].astype(F32)

    def put(c, _):
        scr[pl.ds(OWN + c, SIDE, stride=STRIDE), :] = block(acc, c)
        return 0

    lax.fori_loop(0, peers, put, 0)

    def narrow(i, _):
        buf[i] = scr[pl.ds(i * STRIDE, PITCH), :].astype(BF16)
        return 0

    lax.fori_loop(0, SIDE, narrow, 0, unroll=4)


def zero(ref, blocks):
    def one(c, _):
        ref[pl.ds(pl.multiple_of(c * SIDE, SIDE), SIDE), :] = jnp.zeros((SIDE, SIDE), F32)
        return 0

    lax.fori_loop(0, blocks, one, 0)


def back_dot(tile, y):
    return lax.dot_general(tile, y, (((0,), (0,)), ((), ())), preferred_element_type=F32)


STEP = 8


def first_kernel(
    count, rows, peers_ref, need_ref, tiles, x_ref, y_ref, buf, slots, scr, acc, slot_v, sem
):
    live = count[0]
    row_at = lax.broadcasted_iota(jnp.int32, (SIDE, SIDE), 0)
    lane_at = lax.broadcasted_iota(jnp.int32, (SIDE, SIDE), 1)
    hit = jnp.where((row_at == peers_ref[...]) & (lane_at < live), 1.0, 0.0)
    used = jnp.broadcast_to(jnp.max(hit, axis=1, keepdims=True), (SIDE, SIDE))
    below = jnp.where(lane_at < row_at, 1.0, 0.0).astype(BF16)
    slot = jnp.dot(below, used.astype(BF16), preferred_element_type=F32)
    total = jnp.sum(used, axis=0, keepdims=True)
    lane = lax.broadcasted_iota(jnp.int32, (1, SIDE), 1)
    mine = jnp.sum(hit * slot, axis=0, keepdims=True)
    mine = jnp.where(lane < live, jnp.minimum(mine, float(CAP)), float(CAP))
    peer_total = jnp.minimum(total, float(CAP))
    slot_v[0:1, :] = mine.astype(jnp.int32)
    slot_v[1:2, :] = peer_total.astype(jnp.int32)
    copy = pltpu.make_async_copy(slot_v, slots, sem)
    copy.start()
    at = jnp.where(used > 0, slot, -1.0)
    pick = at == lane_at.astype(F32)
    peer_of = jnp.sum(jnp.where(pick, row_at.astype(F32), 0.0), axis=0, keepdims=True)
    peer_of = jnp.where(lane.astype(F32) < total, peer_of, float(SIDE))
    need_col = jnp.sum(
        jnp.where(row_at == lane_at, need_ref[...], 0).astype(F32), axis=1, keepdims=True
    )
    pick = (at == (lane_at - CAP - 1).astype(F32)) & (lane_at > CAP)
    need_of = jnp.sum(jnp.where(pick, need_col, 0.0), axis=0, keepdims=True)
    meta = jnp.where(lane < CAP, peer_of, jnp.where(lane == CAP, total, need_of))
    scr[pl.ds(META, SIDE, stride=STRIDE), :] = jnp.broadcast_to(meta, (SIDE, SIDE))
    copy.wait()
    peers = slots[1, 0]
    zero(acc, peers)

    def step(g, _):
        parts = []
        for k in range(STEP):
            t = g * STEP + k
            parts.append((slots[0, t], back_dot(tiles[t], block(y_ref, rows[t]))))
        for s, part in parts:
            where = pl.ds(pl.multiple_of(s * SIDE, SIDE), SIDE)
            acc[where, :] = acc[where, :] + part
        return 0

    lax.fori_loop(0, (live + STEP - 1) // STEP, step, 0)
    pack_rows(scr, x_ref, acc, peers, buf)


LOG = CAP.bit_length()
LIST = SIDE * (CAP + 1) // 8 + 8
SUMS = OWN * SIDE + 8


def middle_kernel(total, batches, index, recv, buf, both, parts, outs):
    def load(d, _):
        at = pl.multiple_of(d * OWN, OWN)
        both[pl.ds(at, OWN), :] = recv[d, 0:OWN, :].astype(F32)
        both[pl.ds(SUMS + at, OWN), :] = jnp.zeros((OWN, SIDE), F32)
        return 0

    lax.fori_loop(0, SIDE, load, 0, unroll=4)
    both[OWN * SIDE : SUMS, :] = jnp.zeros((8, SIDE), F32)

    def ahead(k):
        first = pl.multiple_of(batches[k], 8)
        return first, [index[first + j] for j in range(8)]

    def batch(slot, first, spots):
        d = jnp.minimum(lax.shift_right_logical(first, LOG), SIDE - 1)
        start = pl.multiple_of(OWN + (first & CAP), 8)
        parts[slot : slot + 8, :] = recv[d, pl.ds(start, 8), :].astype(F32)
        sums = []
        for j, spot in enumerate(spots):
            outs[pl.ds(first + j, 1), :] = both[pl.ds(spot, 1), :]
            sums.append(both[pl.ds(spot + SUMS, 1), :] + parts[slot + j : slot + j + 1, :])
        for j, spot in enumerate(spots):
            both[pl.ds(spot + SUMS, 1), :] = sums[j]

    def step(g, now):
        other = ahead(2 * g + 1)
        batch(0, *now)
        later = ahead(2 * g + 2)
        batch(8, *other)
        return later

    lax.fori_loop(0, (total[0] + 1) // 2, step, ahead(0))

    def narrow(d, _):
        at = pl.multiple_of(SUMS + d * OWN, 8)
        buf[d, 0:OWN, :] = both[pl.ds(at, OWN), :].astype(BF16)
        at = pl.ds(pl.multiple_of(d * (CAP + 1), CAP + 1), CAP + 1)
        buf[d, OWN:PITCH, :] = outs[at, :].astype(BF16)
        return 0

    lax.fori_loop(0, SIDE, narrow, 0, unroll=4)


def batch_list(counts):
    entries = SIDE * (CAP + 1)
    eights = (counts + 7) // 8
    order = jnp.arange(SIDE, dtype=jnp.int32)
    ends = jnp.sum(jnp.where(order[None, :] <= order[:, None], eights[None, :], 0), axis=1)
    k = jnp.arange(LIST, dtype=jnp.int32)
    before = ends[None, :] <= k[:, None]
    device = jnp.sum(before.astype(jnp.int32), axis=1)
    start = jnp.sum(jnp.where(before, eights[None, :], 0), axis=1)
    return jnp.minimum(device * (CAP + 1) + (k - start) * 8, entries), ends[-1:]


def tail_kernel(
    last, count, rows, slots, recv, tiles, source, target, *rest
):
    if last:
        x_new, y_new, scr, xb, acc_x = rest
        buf = acc = None
    else:
        buf, scr, xb, acc_x, acc, x_new, y_new = rest
    live = count[0]
    peers = slots[1, 0]

    def widen(i, _):
        scr[pl.ds(i * STRIDE, PITCH), :] = recv[i].astype(F32)
        return 0

    lax.fori_loop(0, SIDE, widen, 0, unroll=4)
    for b in range(OWN):
        at = slice(b * SIDE, (b + 1) * SIDE)
        y_new[at, :] = settle(target[at, :], scr[pl.ds(b, SIDE, stride=STRIDE), :])

    def fetch(c, _):
        xb[pl.ds(pl.multiple_of(c * SIDE, SIDE), SIDE), :] = scr[
            pl.ds(OWN + c, SIDE, stride=STRIDE), :
        ].astype(BF16)
        return 0

    lax.fori_loop(0, peers, fetch, 0)
    zero(acc_x, OWN)
    if not last:
        zero(acc, peers)

    def step(g, _):
        ahead, back = [], []
        for k in range(STEP):
            t = g * STEP + k
            s, r, tile = slots[0, t], rows[t], tiles[t]
            to = jnp.where(t < live, r, OWN)
            ahead.append((to, jnp.dot(tile, block(xb, s), preferred_element_type=F32)))
            if not last:
                back.append((s, back_dot(tile, block(y_new, r))))
        for ref, found in ((acc_x, ahead), (acc, back)):
            for s, part in found:
                where = pl.ds(pl.multiple_of(s * SIDE, SIDE), SIDE)
                ref[where, :] = ref[where, :] + part
        return 0

    lax.fori_loop(0, (live + STEP - 1) // STEP, step, 0)
    for b in range(OWN):
        at = slice(b * SIDE, (b + 1) * SIDE)
        x_new[at, :] = settle(source[at, :], acc_x[at, :])
    if not last:
        pack_rows(scr, x_new, acc, peers, buf)


def vmem(shape, dtype):
    return pltpu.VMEM(shape, dtype)


IN_VMEM = pl.BlockSpec(memory_space=pltpu.VMEM)
IN_SMEM = pl.BlockSpec(memory_space=pltpu.SMEM)
BUF = jax.ShapeDtypeStruct((SIDE, PITCH, SIDE), BF16)
NODES = jax.ShapeDtypeStruct((OWN * SIDE, SIDE), BF16)


def fast(source, target, tile_values, tile_rows, tile_peers, need_list, tile_count):
    swap = lambda value: lax.all_to_all(value, "rows", split_axis=0, concat_axis=0, tiled=True)
    buf, slots = pl.pallas_call(
        first_kernel,
        out_shape=(BUF, jax.ShapeDtypeStruct((8, SIDE), jnp.int32)),
        in_specs=[IN_SMEM] * 2 + [IN_VMEM] * 5,
        out_specs=(IN_VMEM, IN_SMEM),
        scratch_shapes=[
            vmem((SIDE * STRIDE, SIDE), F32),
            vmem(((CAP + 1) * SIDE, SIDE), F32),
            vmem((8, SIDE), jnp.int32),
            pltpu.SemaphoreType.DMA,
        ],
        compiler_params=pltpu.CompilerParams(vmem_limit_bytes=28 * MIB),
        name="first",
    )(
        tile_count,
        tile_rows,
        tile_peers.reshape(1, SIDE),
        need_list.reshape(1, SIDE),
        tile_values,
        source,
        target,
    )
    recv = swap(buf)
    meta = recv[:, META, :].astype(F32)
    counts = meta[:, CAP].astype(jnp.int32)
    spots = (meta[:, :CAP] * OWN + meta[:, CAP + 1 : 2 * CAP + 1]).astype(jnp.int32)
    index = jnp.pad(spots, ((0, 0), (0, 1)), constant_values=OWN * SIDE).reshape(-1)
    index = jnp.pad(index, (0, 8), constant_values=OWN * SIDE)
    batches, total = batch_list(jnp.minimum(counts, CAP))
    middle = pl.pallas_call(
        middle_kernel,
        out_shape=BUF,
        in_specs=[IN_SMEM] * 3 + [IN_VMEM],
        out_specs=IN_VMEM,
        scratch_shapes=[
            vmem((2 * SUMS, SIDE), F32),
            vmem((16, SIDE), F32),
            vmem((SIDE * (CAP + 1) + 8, SIDE), F32),
        ],
        compiler_params=pltpu.CompilerParams(vmem_limit_bytes=28 * MIB),
        name="middle",
    )
    for iteration in range(ITERS):
        recv = swap(middle(total, batches, index, recv))
        last = iteration == ITERS - 1
        wide = vmem((SIDE * STRIDE, SIDE), F32)
        xb = vmem(((CAP + 1) * SIDE, SIDE), BF16)
        acc_x = vmem(((OWN + 1) * SIDE, SIDE), F32)
        acc = vmem(((CAP + 1) * SIDE, SIDE), F32)
        node = vmem((OWN * SIDE, SIDE), BF16)
        out = pl.pallas_call(
            functools.partial(tail_kernel, last),
            out_shape=(NODES, NODES) if last else BUF,
            in_specs=[IN_SMEM] * 3 + [IN_VMEM] * 4,
            out_specs=(IN_VMEM, IN_VMEM) if last else IN_VMEM,
            scratch_shapes=[wide, xb, acc_x] if last else [wide, xb, acc_x, acc, node, node],
            compiler_params=pltpu.CompilerParams(vmem_limit_bytes=32 * MIB),
            name="last" if last else "tail",
        )(tile_count, tile_rows, slots, recv, tile_values, source, target)
        if not last:
            recv = swap(out)
    return out, jnp.max(counts) > CAP


def general(source, target, tile_values, tile_rows, tile_peers, need_list, tile_count):
    peers_total = lax.axis_size("rows")
    row_count = source.shape[0] // SIDE
    tiles_here = tile_values.shape[0]
    group = min(16, tiles_here)
    live = (jnp.arange(tiles_here, dtype=jnp.int32) < tile_count[0]).astype(F32)[:, None, None]
    swap = lambda value: lax.all_to_all(value, "rows", split_axis=0, concat_axis=0, tiled=True)
    send_list = swap(need_list.reshape(peers_total, 1))[:, 0]
    owner_hot = (send_list[None, :] == jnp.arange(row_count, dtype=jnp.int32)[:, None]).astype(F32)

    def take(value, position):
        return lax.dynamic_slice_in_dim(value, position * group, group, 0)

    def product(form, vectors, position, ids):
        return (
            jnp.einsum(form, take(tile_values, position), vectors[ids], preferred_element_type=F32)
            * take(live, position)
        )

    def iterate(_, state):
        source_now, target_now = state
        source_blocks = source_now.reshape(row_count, SIDE, SIDE)
        target_blocks = target_now.reshape(row_count, SIDE, SIDE)

        def backward(position, running):
            part = product("tji,tjk->tik", target_blocks, position, take(tile_rows, position))
            return running.at[take(tile_peers, position)].add(part)

        partial = lax.fori_loop(
            0, tiles_here // group, backward, jnp.zeros((peers_total, SIDE, SIDE), F32)
        )
        both = swap(jnp.stack([source_blocks[send_list], partial.astype(BF16)], axis=1))
        fetched = both[:, 0]

        def forward(position, running):
            part = product("tij,tjk->tik", fetched, position, take(tile_peers, position))
            return running.at[take(tile_rows, position)].add(part)

        gathered = lax.fori_loop(
            0, tiles_here // group, forward, jnp.zeros((row_count, SIDE, SIDE), F32)
        )
        incoming = jnp.dot(
            owner_hot,
            both[:, 1].astype(F32).reshape(peers_total, -1),
            precision=lax.Precision.HIGHEST,
            preferred_element_type=F32,
        )
        return (
            settle(source, gathered.reshape(-1, SIDE)),
            settle(target, incoming.reshape(-1, SIDE)),
        )

    return lax.fori_loop(0, ITERS, iterate, (source, target))


def shards(*args):
    found, over = fast(*args)
    return lax.cond(over, lambda: general(*args), lambda: found)


def solution(mesh):
    return jax.shard_map(
        shards,
        mesh=mesh,
        in_specs=(
            P("rows", None),
            P("rows", None),
            P("rows", None, None),
            P("rows"),
            P("rows"),
            P("rows", None),
            P("rows"),
        ),
        out_specs=(P("rows", None), P("rows", None)),
        check_vma=False,
    )
```

```python
import functools
import jax
import jax.numpy as jnp
from jax import lax
from jax.experimental import pallas as pl
from jax.experimental.pallas import tpu as pltpu
from jax.sharding import PartitionSpec as P

ITERS = 2
epsilon = 1e-06

SIDE = 128
OWN = 16
CAP = 63
PITCH = OWN + CAP + 1
META = PITCH - 1
STRIDE = PITCH + 1
F32 = jnp.float32
BF16 = jnp.bfloat16
MIB = 1 << 20


def settle(base, update):
    total = base.astype(F32) + update
    scale = lax.rsqrt(jnp.mean(total * total, axis=-1, keepdims=True) + epsilon)
    return (total * scale).astype(BF16)


def block(ref, index):
    return ref[pl.ds(pl.multiple_of(index * SIDE, SIDE), SIDE), :]


def pack_rows(scr, x_ref, acc, peers, buf):
    for b in range(OWN):
        scr[pl.ds(b, SIDE, stride=STRIDE), :] = x_ref[b * SIDE : (b + 1) * SIDE, :].astype(F32)

    def put(c, _):
        scr[pl.ds(OWN + c, SIDE, stride=STRIDE), :] = block(acc, c)
        return 0

    lax.fori_loop(0, peers, put, 0)

    def narrow(i, _):
        buf[i] = scr[pl.ds(i * STRIDE, PITCH), :].astype(BF16)
        return 0

    lax.fori_loop(0, SIDE, narrow, 0, unroll=4)


def zero(ref, blocks):
    def one(c, _):
        ref[pl.ds(pl.multiple_of(c * SIDE, SIDE), SIDE), :] = jnp.zeros((SIDE, SIDE), F32)
        return 0

    lax.fori_loop(0, blocks, one, 0)


def back_dot(tile, y):
    return lax.dot_general(tile, y, (((0,), (0,)), ((), ())), preferred_element_type=F32)


STEP = 8
CHUNK = 16


def tile_copy(tiles, held, sems, c):
    at = pl.ds(pl.multiple_of(c * CHUNK, CHUNK), CHUNK)
    return pltpu.make_async_copy(tiles.at[at], held.at[at], sems.at[c])


def start_tiles(tiles, held, sems):
    for c in range(SIDE // CHUNK):
        tile_copy(tiles, held, sems, c).start()


def over_tiles(live, step, tiles=None, held=None, sems=None):
    if tiles is None:
        lax.fori_loop(0, (live + STEP - 1) // STEP, step, 0)
        return

    def chunk(c, _):
        tile_copy(tiles, held, sems, c).wait()
        first = c * (CHUNK // STEP)
        end = jnp.minimum((live + STEP - 1) // STEP, first + CHUNK // STEP)
        lax.fori_loop(first, end, step, 0)
        return 0

    lax.fori_loop(0, SIDE // CHUNK, chunk, 0)


def first_kernel(
    count, rows, peers_ref, need_ref, hbm, x_ref, y_ref, buf, slots, scr, acc, slot_v, sem, tiles, sems
):
    start_tiles(hbm, tiles, sems)
    live = count[0]
    row_at = lax.broadcasted_iota(jnp.int32, (SIDE, SIDE), 0)
    lane_at = lax.broadcasted_iota(jnp.int32, (SIDE, SIDE), 1)
    hit = jnp.where((row_at == peers_ref[...]) & (lane_at < live), 1.0, 0.0)
    used = jnp.broadcast_to(jnp.max(hit, axis=1, keepdims=True), (SIDE, SIDE))
    below = jnp.where(lane_at < row_at, 1.0, 0.0).astype(BF16)
    slot = jnp.dot(below, used.astype(BF16), preferred_element_type=F32)
    total = jnp.sum(used, axis=0, keepdims=True)
    lane = lax.broadcasted_iota(jnp.int32, (1, SIDE), 1)
    mine = jnp.sum(hit * slot, axis=0, keepdims=True)
    mine = jnp.where(lane < live, jnp.minimum(mine, float(CAP)), float(CAP))
    peer_total = jnp.minimum(total, float(CAP))
    slot_v[0:1, :] = mine.astype(jnp.int32)
    slot_v[1:2, :] = peer_total.astype(jnp.int32)
    copy = pltpu.make_async_copy(slot_v, slots, sem)
    copy.start()
    at = jnp.where(used > 0, slot, -1.0)
    pick = at == lane_at.astype(F32)
    peer_of = jnp.sum(jnp.where(pick, row_at.astype(F32), 0.0), axis=0, keepdims=True)
    peer_of = jnp.where(lane.astype(F32) < total, peer_of, float(SIDE))
    need_col = jnp.sum(
        jnp.where(row_at == lane_at, need_ref[...], 0).astype(F32), axis=1, keepdims=True
    )
    pick = (at == (lane_at - CAP - 1).astype(F32)) & (lane_at > CAP)
    need_of = jnp.sum(jnp.where(pick, need_col, 0.0), axis=0, keepdims=True)
    meta = jnp.where(lane < CAP, peer_of, jnp.where(lane == CAP, total, need_of))
    scr[pl.ds(META, SIDE, stride=STRIDE), :] = jnp.broadcast_to(meta, (SIDE, SIDE))
    copy.wait()
    peers = slots[1, 0]
    zero(acc, peers)

    def step(g, _):
        parts = []
        for k in range(STEP):
            t = g * STEP + k
            parts.append((slots[0, t], back_dot(tiles[t], block(y_ref, rows[t]))))
        for s, part in parts:
            where = pl.ds(pl.multiple_of(s * SIDE, SIDE), SIDE)
            acc[where, :] = acc[where, :] + part
        return 0

    over_tiles(live, step, hbm, tiles, sems)
    pack_rows(scr, x_ref, acc, peers, buf)


LOG = CAP.bit_length()
LIST = SIDE * (CAP + 1) // 8 + 8
PAD = 8
DUMMY = OWN * SIDE
SUMS = PAD + DUMMY + 16


def middle_kernel(batches, index, recv, buf, both):
    def load(d, _):
        at = pl.multiple_of(PAD + d * OWN, 8)
        both[pl.ds(at, OWN), :] = recv[d, 0:OWN, :].astype(F32)
        both[pl.ds(SUMS + at, OWN), :] = jnp.zeros((OWN, SIDE), F32)
        return 0

    lax.fori_loop(0, SIDE, load, 0, unroll=4)
    row_at = lax.broadcasted_iota(jnp.int32, (8, SIDE), 0)

    def batch(first, spots):
        d = lax.shift_right_logical(first, LOG)
        start = pl.multiple_of(OWN + (first & CAP), 8)
        parts = recv[d, pl.ds(start, 8), :].astype(F32)
        picked = both[pl.ds(spots[0] + PAD, 8), :]
        sums = []
        for j, spot in enumerate(spots):
            if j:
                picked = jnp.where(row_at == j, both[pl.ds(spot + (PAD - j), 8), :], picked)
            sums.append(both[pl.ds(spot + (SUMS + PAD - j), 8), :] + parts)
        buf[d, pl.ds(start, 8), :] = picked.astype(BF16)
        for j, spot in enumerate(spots):
            window = both.at[pl.ds(spot + (SUMS + PAD - j), 8), :]
            pltpu.store(window, sums[j], mask=row_at == j)

    def ahead(k):
        first = pl.multiple_of(batches[k], 8)
        return first, [index[first + j] for j in range(8)]

    total = batches[LIST - 1]

    def four(g, _):
        for k in range(4):
            batch(*ahead(4 * g + k))
        return 0

    def one(k, _):
        batch(*ahead(k))
        return 0

    fours = lax.shift_right_logical(total, 2)
    lax.fori_loop(0, fours, four, 0)
    lax.fori_loop(4 * fours, total, one, 0)

    def narrow(d, _):
        at = pl.multiple_of(SUMS + PAD + d * OWN, 8)
        buf[d, 0:OWN, :] = both[pl.ds(at, OWN), :].astype(BF16)
        return 0

    lax.fori_loop(0, SIDE, narrow, 0, unroll=4)


def batch_list(counts):
    eights = (counts + 7) // 8
    order = jnp.arange(SIDE, dtype=jnp.int32)
    ends = jnp.sum(jnp.where(order[None, :] <= order[:, None], eights[None, :], 0), axis=1)
    k = jnp.arange(LIST, dtype=jnp.int32)
    total = jnp.sum(eights)
    before = ends[None, :] <= k[:, None]
    device = jnp.sum(before.astype(jnp.int32), axis=1)
    start = jnp.sum(jnp.where(before, eights[None, :], 0), axis=1)
    return jnp.where(k == LIST - 1, total, device * (CAP + 1) + (k - start) * 8)


def tail_kernel(
    last, count, rows, slots, recv, tiles, source, target, *rest
):
    coming = ()
    if last:
        x_new, y_new, scr, xb, acc_x, held, sems = rest
        coming = tiles, held, sems
        start_tiles(*coming)
        buf, acc, tiles = None, None, held
    else:
        buf, scr, xb, acc_x, acc, x_new, y_new = rest
    live = count[0]
    peers = slots[1, 0]

    def widen(i, _):
        scr[pl.ds(i * STRIDE, PITCH), :] = recv[i].astype(F32)
        return 0

    lax.fori_loop(0, SIDE, widen, 0, unroll=4)
    for b in range(OWN):
        at = slice(b * SIDE, (b + 1) * SIDE)
        y_new[at, :] = settle(target[at, :], scr[pl.ds(b, SIDE, stride=STRIDE), :])

    def fetch(c, _):
        xb[pl.ds(pl.multiple_of(c * SIDE, SIDE), SIDE), :] = scr[
            pl.ds(OWN + c, SIDE, stride=STRIDE), :
        ].astype(BF16)
        return 0

    lax.fori_loop(0, peers, fetch, 0)
    zero(acc_x, OWN)
    if not last:
        zero(acc, peers)

    def step(g, _):
        ahead, back = [], []
        for k in range(STEP):
            t = g * STEP + k
            s, r, tile = slots[0, t], rows[t], tiles[t]
            to = jnp.where(t < live, r, OWN)
            ahead.append((to, jnp.dot(tile, block(xb, s), preferred_element_type=F32)))
            if not last:
                back.append((s, back_dot(tile, block(y_new, r))))
        for ref, found in ((acc_x, ahead), (acc, back)):
            for s, part in found:
                where = pl.ds(pl.multiple_of(s * SIDE, SIDE), SIDE)
                ref[where, :] = ref[where, :] + part
        return 0

    over_tiles(live, step, *coming)
    for b in range(OWN):
        at = slice(b * SIDE, (b + 1) * SIDE)
        x_new[at, :] = settle(source[at, :], acc_x[at, :])
    if not last:
        pack_rows(scr, x_new, acc, peers, buf)


def vmem(shape, dtype):
    return pltpu.VMEM(shape, dtype)


IN_VMEM = pl.BlockSpec(memory_space=pltpu.VMEM)
IN_SMEM = pl.BlockSpec(memory_space=pltpu.SMEM)
ANYWHERE = pl.BlockSpec(memory_space=pl.ANY)
TILES_HELD = vmem((SIDE, SIDE, SIDE), BF16), pltpu.SemaphoreType.DMA((SIDE // CHUNK,))
BUF = jax.ShapeDtypeStruct((SIDE, PITCH, SIDE), BF16)
NODES = jax.ShapeDtypeStruct((OWN * SIDE, SIDE), BF16)


def fast(source, target, tile_values, tile_rows, tile_peers, need_list, tile_count):
    swap = lambda value: lax.all_to_all(value, "rows", split_axis=0, concat_axis=0, tiled=True)
    buf, slots = pl.pallas_call(
        first_kernel,
        out_shape=(BUF, jax.ShapeDtypeStruct((8, SIDE), jnp.int32)),
        in_specs=[IN_SMEM] * 2 + [IN_VMEM] * 2 + [ANYWHERE] + [IN_VMEM] * 2,
        out_specs=(IN_VMEM, IN_SMEM),
        scratch_shapes=[
            vmem((SIDE * STRIDE, SIDE), F32),
            vmem(((CAP + 1) * SIDE, SIDE), F32),
            vmem((8, SIDE), jnp.int32),
            pltpu.SemaphoreType.DMA,
            *TILES_HELD,
        ],
        compiler_params=pltpu.CompilerParams(vmem_limit_bytes=28 * MIB),
        name="first",
    )(
        tile_count,
        tile_rows,
        tile_peers.reshape(1, SIDE),
        need_list.reshape(1, SIDE),
        tile_values,
        source,
        target,
    )
    recv = swap(buf)
    meta = recv[:, META, :].astype(F32)
    counts = meta[:, CAP].astype(jnp.int32)
    spots = (meta[:, :CAP] * OWN + meta[:, CAP + 1 : 2 * CAP + 1]).astype(jnp.int32)
    index = jnp.pad(spots, ((0, 0), (0, 1)), constant_values=DUMMY).reshape(-1)
    batches = batch_list(jnp.minimum(counts, CAP))
    middle = pl.pallas_call(
        middle_kernel,
        out_shape=BUF,
        in_specs=[IN_SMEM] * 2 + [IN_VMEM],
        out_specs=IN_VMEM,
        scratch_shapes=[vmem((2 * SUMS, SIDE), F32)],
        compiler_params=pltpu.CompilerParams(vmem_limit_bytes=16 * MIB),
        name="middle",
    )
    for iteration in range(ITERS):
        recv = swap(middle(batches, index, recv))
        last = iteration == ITERS - 1
        wide = vmem((SIDE * STRIDE, SIDE), F32)
        xb = vmem(((CAP + 1) * SIDE, SIDE), BF16)
        acc_x = vmem(((OWN + 1) * SIDE, SIDE), F32)
        acc = vmem(((CAP + 1) * SIDE, SIDE), F32)
        node = vmem((OWN * SIDE, SIDE), BF16)
        out = pl.pallas_call(
            functools.partial(tail_kernel, last),
            out_shape=(NODES, NODES) if last else BUF,
            in_specs=[IN_SMEM] * 3 + [IN_VMEM, ANYWHERE if last else IN_VMEM] + [IN_VMEM] * 2,
            out_specs=(IN_VMEM, IN_VMEM) if last else IN_VMEM,
            scratch_shapes=[wide, xb, acc_x, *(TILES_HELD if last else (acc, node, node))],
            compiler_params=pltpu.CompilerParams(vmem_limit_bytes=32 * MIB),
            name="last" if last else "tail",
        )(tile_count, tile_rows, slots, recv, tile_values, source, target)
        if not last:
            recv = swap(out)
    return out, jnp.max(counts) > CAP


def general(source, target, tile_values, tile_rows, tile_peers, need_list, tile_count):
    peers_total = lax.axis_size("rows")
    row_count = source.shape[0] // SIDE
    tiles_here = tile_values.shape[0]
    group = min(16, tiles_here)
    live = (jnp.arange(tiles_here, dtype=jnp.int32) < tile_count[0]).astype(F32)[:, None, None]
    swap = lambda value: lax.all_to_all(value, "rows", split_axis=0, concat_axis=0, tiled=True)
    send_list = swap(need_list.reshape(peers_total, 1))[:, 0]
    owner_hot = (send_list[None, :] == jnp.arange(row_count, dtype=jnp.int32)[:, None]).astype(F32)

    def take(value, position):
        return lax.dynamic_slice_in_dim(value, position * group, group, 0)

    def product(form, vectors, position, ids):
        return (
            jnp.einsum(form, take(tile_values, position), vectors[ids], preferred_element_type=F32)
            * take(live, position)
        )

    def iterate(_, state):
        source_now, target_now = state
        source_blocks = source_now.reshape(row_count, SIDE, SIDE)
        target_blocks = target_now.reshape(row_count, SIDE, SIDE)

        def backward(position, running):
            part = product("tji,tjk->tik", target_blocks, position, take(tile_rows, position))
            return running.at[take(tile_peers, position)].add(part)

        partial = lax.fori_loop(
            0, tiles_here // group, backward, jnp.zeros((peers_total, SIDE, SIDE), F32)
        )
        both = swap(jnp.stack([source_blocks[send_list], partial.astype(BF16)], axis=1))
        fetched = both[:, 0]

        def forward(position, running):
            part = product("tij,tjk->tik", fetched, position, take(tile_peers, position))
            return running.at[take(tile_rows, position)].add(part)

        gathered = lax.fori_loop(
            0, tiles_here // group, forward, jnp.zeros((row_count, SIDE, SIDE), F32)
        )
        incoming = jnp.dot(
            owner_hot,
            both[:, 1].astype(F32).reshape(peers_total, -1),
            precision=lax.Precision.HIGHEST,
            preferred_element_type=F32,
        )
        return (
            settle(source, gathered.reshape(-1, SIDE)),
            settle(target, incoming.reshape(-1, SIDE)),
        )

    return lax.fori_loop(0, ITERS, iterate, (source, target))


def shards(*args):
    found, over = fast(*args)
    return lax.cond(over, lambda: general(*args), lambda: found)


def solution(mesh):
    return jax.shard_map(
        shards,
        mesh=mesh,
        in_specs=(
            P("rows", None),
            P("rows", None),
            P("rows", None, None),
            P("rows"),
            P("rows"),
            P("rows", None),
            P("rows"),
        ),
        out_specs=(P("rows", None), P("rows", None)),
        check_vma=False,
    )
```

```python
import functools
import jax
import jax.numpy as jnp
from jax import lax
from jax.experimental import pallas as pl
from jax.experimental.pallas import tpu as pltpu
from jax.sharding import PartitionSpec as P

ITERS = 2
epsilon = 1e-06

SIDE = 128
OWN = 16
CAP = 63
FEW = 56
PITCH = OWN + CAP + 1
META = PITCH - 1
F32 = jnp.float32
BF16 = jnp.bfloat16
MIB = 1 << 20


def settle(base, update):
    total = base.astype(F32) + update
    scale = lax.rsqrt(jnp.mean(total * total, axis=-1, keepdims=True) + epsilon)
    return (total * scale).astype(BF16)


def block(ref, index):
    return ref[pl.ds(pl.multiple_of(index * SIDE, SIDE), SIDE), :]


def odd_pitch(pitch):
    return pitch + 1


def pack_rows(pitch, scr, x_ref, acc, peers, buf):
    stride = odd_pitch(pitch)
    for b in range(OWN):
        scr[pl.ds(b, SIDE, stride=stride), :] = x_ref[b * SIDE : (b + 1) * SIDE, :].astype(F32)

    def put(c, _):
        scr[pl.ds(OWN + c, SIDE, stride=stride), :] = block(acc, c)
        return 0

    lax.fori_loop(0, peers, put, 0)

    def narrow(i, _):
        buf[i] = scr[pl.ds(i * stride, pitch), :].astype(BF16)
        return 0

    lax.fori_loop(0, SIDE, narrow, 0, unroll=4)


def zero(ref, blocks):
    def one(c, _):
        ref[pl.ds(pl.multiple_of(c * SIDE, SIDE), SIDE), :] = jnp.zeros((SIDE, SIDE), F32)
        return 0

    lax.fori_loop(0, blocks, one, 0)


def back_dot(tile, y):
    return lax.dot_general(tile, y, (((0,), (0,)), ((), ())), preferred_element_type=F32)


STEP = 8
CHUNK = 16


def tile_copy(tiles, held, sems, c):
    at = pl.ds(pl.multiple_of(c * CHUNK, CHUNK), CHUNK)
    return pltpu.make_async_copy(tiles.at[at], held.at[at], sems.at[c])


def start_tiles(tiles, held, sems):
    for c in range(SIDE // CHUNK):
        tile_copy(tiles, held, sems, c).start()


def over_tiles(live, step, tiles=None, held=None, sems=None):
    if tiles is None:
        lax.fori_loop(0, (live + STEP - 1) // STEP, step, 0)
        return

    def chunk(c, _):
        tile_copy(tiles, held, sems, c).wait()
        first = c * (CHUNK // STEP)
        end = jnp.minimum((live + STEP - 1) // STEP, first + CHUNK // STEP)
        lax.fori_loop(first, end, step, 0)
        return 0

    lax.fori_loop(0, SIDE // CHUNK, chunk, 0)


def first_kernel(
    count, rows, peers_ref, need_ref, rows_ref, hbm, source, target, *rest
):
    buf, slots, x_ref, y_ref, scr, acc, slot_v, sem, tiles, sems, node_sems = rest
    y_copy = pltpu.make_async_copy(target, y_ref, node_sems.at[0])
    x_copy = pltpu.make_async_copy(source, x_ref, node_sems.at[1])
    y_copy.start()
    start_tiles(hbm, tiles, sems)
    x_copy.start()
    live = count[0]
    row_at = lax.broadcasted_iota(jnp.int32, (SIDE, SIDE), 0)
    lane_at = lax.broadcasted_iota(jnp.int32, (SIDE, SIDE), 1)
    hit = jnp.where((row_at == peers_ref[...]) & (lane_at < live), 1.0, 0.0)
    used = jnp.broadcast_to(jnp.max(hit, axis=1, keepdims=True), (SIDE, SIDE))
    below = jnp.where(lane_at < row_at, 1.0, 0.0).astype(BF16)
    slot = jnp.dot(below, used.astype(BF16), preferred_element_type=F32)
    total = jnp.sum(used, axis=0, keepdims=True)
    lane = lax.broadcasted_iota(jnp.int32, (1, SIDE), 1)
    mine = jnp.sum(hit * slot, axis=0, keepdims=True)
    mine = jnp.where(lane < live, jnp.minimum(mine, float(CAP)), float(CAP))
    peer_total = jnp.minimum(total, float(CAP))
    slot_v[0:1, :] = mine.astype(jnp.int32)
    slot_v[1:2, :] = peer_total.astype(jnp.int32)
    slot_v[2:3, :] = rows_ref[...]
    slot_v[3:4, :] = jnp.zeros((1, SIDE), jnp.int32) + live
    copy = pltpu.make_async_copy(slot_v, slots, sem)
    copy.start()
    order = lane_at & CAP
    order = ((order & 7) * 8 + lax.shift_right_logical(order, 3)).astype(F32)
    pick = (used > 0) & (slot == order)
    peer_of = jnp.sum(jnp.where(pick, row_at.astype(F32), 0.0), axis=0, keepdims=True)
    peer_of = jnp.where(order[0:1, :] < total, peer_of, float(SIDE))
    need_col = jnp.sum(
        jnp.where(row_at == lane_at, need_ref[...], 0).astype(F32), axis=1, keepdims=True
    )
    need_of = jnp.sum(jnp.where(pick, need_col, 0.0), axis=0, keepdims=True)
    meta = jnp.where(lane < CAP, peer_of, jnp.where(lane == CAP, total, need_of))
    scr[pl.ds(META, SIDE, stride=odd_pitch(PITCH)), :] = jnp.broadcast_to(meta, (SIDE, SIDE))
    copy.wait()
    peers = slots[1, 0]
    zero(acc, peers)
    y_copy.wait()

    def step(g, _):
        parts = []
        for k in range(STEP):
            t = g * STEP + k
            parts.append((slots[0, t], back_dot(tiles[t], block(y_ref, rows[t]))))
        for s, part in parts:
            where = pl.ds(pl.multiple_of(s * SIDE, SIDE), SIDE)
            acc[where, :] = acc[where, :] + part
        return 0

    over_tiles(live, step, hbm, tiles, sems)
    x_copy.wait()
    pack_rows(PITCH, scr, x_ref, acc, peers, buf)


GROUPS = SIDE * (CAP + 1) // 8
PAD = 8
DUMMY = OWN * SIDE
SUMS = PAD + DUMMY + 16


def middle_kernel(*refs):
    *index, onward, recv, buf, even, odd = refs

    def load(d, _):
        at = pl.multiple_of(PAD + d * OWN, 8)
        rows = recv[d, 0:OWN, :].astype(F32)
        for ref in (even, odd):
            ref[pl.ds(at, OWN), :] = rows
            ref[pl.ds(SUMS + at, OWN), :] = jnp.zeros((OWN, SIDE), F32)
        return 0

    lax.fori_loop(0, SIDE, load, 0, unroll=4)
    row_at = lax.broadcasted_iota(jnp.int32, (8, SIDE), 0)

    def clip(group):
        return jnp.where(group < GROUPS, group, GROUPS - 8)

    def after(group):
        return group + onward[clip(group)]

    def work(groups):
        jobs = []
        for ref, group in zip((even, odd), groups):
            spots = [entry[clip(group)] for entry in index]
            d = lax.shift_right_logical(clip(group), 3)
            at = d, pl.ds(pl.multiple_of(OWN + (clip(group) & 7) * 8, 8), 8), slice(None)
            parts = jnp.where(group >= GROUPS, 0.0, recv[at].astype(F32))
            jobs.append((ref, spots, at, parts))
        found = []
        for ref, spots, at, parts in jobs:
            picked = ref[pl.ds(spots[0] + PAD, 8), :]
            sums = [ref[pl.ds(spots[0] + SUMS + PAD, 8), :] + parts]
            for j in range(1, 8):
                picked = jnp.where(row_at == j, ref[pl.ds(spots[j] + PAD - j, 8), :], picked)
                sums.append(ref[pl.ds(spots[j] + (SUMS + PAD - j), 8), :] + parts)
            found.append((picked, sums))
        for (ref, spots, at, _), (picked, sums) in zip(jobs, found):
            buf[at] = picked.astype(BF16)
            for j, spot in enumerate(spots):
                window = ref.at[pl.ds(spot + (SUMS + PAD - j), 8), :]
                pltpu.store(window, sums[j], mask=row_at == j)

    def two(groups):
        first = after(groups[1])
        second = after(first)
        third = after(second)
        fourth = after(third)
        work(groups)
        work((first, second))
        return third, fourth

    lax.while_loop(lambda groups: groups[0] < GROUPS, two, (jnp.int32(0), after(jnp.int32(0))))

    def narrow(d, _):
        at = pl.ds(pl.multiple_of(SUMS + PAD + d * OWN, 8), OWN)
        buf[d, 0:OWN, :] = (even[at, :] + odd[at, :]).astype(BF16)
        return 0

    lax.fori_loop(0, SIDE, narrow, 0, unroll=4)


def tail_kernel(
    last, pitch, slots, recv, tiles, source, target, *rest
):
    if last:
        x_new, y_new, scr, xb, acc_x = rest
        buf = acc = None
    else:
        buf, scr, xb, acc_x, acc, x_new, y_new = rest
    live = slots[3, 0]
    peers = slots[1, 0]
    stride = odd_pitch(pitch)

    def widen(i, _):
        scr[pl.ds(i * stride, pitch), :] = recv[i].astype(F32)
        return 0

    lax.fori_loop(0, SIDE, widen, 0, unroll=4)
    for b in range(OWN):
        at = slice(b * SIDE, (b + 1) * SIDE)
        y_new[at, :] = settle(target[at, :], scr[pl.ds(b, SIDE, stride=stride), :])

    def fetch(c, _):
        xb[pl.ds(pl.multiple_of(c * SIDE, SIDE), SIDE), :] = scr[
            pl.ds(OWN + c, SIDE, stride=stride), :
        ].astype(BF16)
        return 0

    lax.fori_loop(0, peers, fetch, 0)
    zero(acc_x, OWN)
    if not last:
        zero(acc, peers)

    def step(g, _):
        ahead, back = [], []
        for k in range(STEP):
            t = g * STEP + k
            s, r, tile = slots[0, t], slots[2, t], tiles[t]
            to = jnp.where(t < live, r, OWN)
            ahead.append((to, jnp.dot(tile, block(xb, s), preferred_element_type=F32)))
            if not last:
                back.append((s, back_dot(tile, block(y_new, r))))
        for ref, found in ((acc_x, ahead), (acc, back)):
            for s, part in found:
                where = pl.ds(pl.multiple_of(s * SIDE, SIDE), SIDE)
                ref[where, :] = ref[where, :] + part
        return 0

    over_tiles(live, step)
    for b in range(OWN):
        at = slice(b * SIDE, (b + 1) * SIDE)
        x_new[at, :] = settle(source[at, :], acc_x[at, :])
    if not last:
        pack_rows(pitch, scr, x_new, acc, peers, buf)


def vmem(shape, dtype):
    return pltpu.VMEM(shape, dtype)


IN_VMEM = pl.BlockSpec(memory_space=pltpu.VMEM)
IN_SMEM = pl.BlockSpec(memory_space=pltpu.SMEM)
ANYWHERE = pl.BlockSpec(memory_space=pl.ANY)
NODES = jax.ShapeDtypeStruct((OWN * SIDE, SIDE), BF16)


def buffer(pitch):
    return jax.ShapeDtypeStruct((SIDE, pitch, SIDE), BF16)


def wide(pitch):
    return vmem((SIDE * odd_pitch(pitch), SIDE), F32)


def swap(value):
    return lax.all_to_all(value, "rows", split_axis=0, concat_axis=0, tiled=True)


def begin(source, target, tile_values, tile_rows, tile_peers, need_list, tile_count):
    buf, slots, *kept = pl.pallas_call(
        first_kernel,
        out_shape=(buffer(PITCH), jax.ShapeDtypeStruct((8, SIDE), jnp.int32), NODES, NODES),
        in_specs=[IN_SMEM] * 2 + [IN_VMEM] * 3 + [ANYWHERE] * 3,
        out_specs=(IN_VMEM, IN_SMEM, IN_VMEM, IN_VMEM),
        scratch_shapes=[
            wide(PITCH),
            vmem(((CAP + 1) * SIDE, SIDE), F32),
            vmem((8, SIDE), jnp.int32),
            pltpu.SemaphoreType.DMA,
            vmem((SIDE, SIDE, SIDE), BF16),
            pltpu.SemaphoreType.DMA((SIDE // CHUNK,)),
            pltpu.SemaphoreType.DMA((2,)),
        ],
        compiler_params=pltpu.CompilerParams(vmem_limit_bytes=28 * MIB),
        name="first",
    )(
        tile_count,
        tile_rows,
        tile_peers.reshape(1, SIDE),
        need_list.reshape(1, SIDE),
        tile_rows.reshape(1, SIDE),
        tile_values,
        source,
        target,
    )
    recv = swap(buf)
    meta = recv[:, META, :].astype(F32)
    most = jnp.max(meta[:, CAP])
    which = (most > FEW).astype(jnp.int32) + (most > CAP).astype(jnp.int32)
    return recv, meta, slots, kept, which, most


def proceed(pitch, recv, meta, slots, source, target, tile_values):
    lane = lax.broadcasted_iota(jnp.int32, (SIDE, CAP + 1), 1)
    spots = meta[:, : CAP + 1] * OWN + meta[:, CAP + 1 :]
    spots = jnp.where(lane == CAP, float(DUMMY), spots)
    peers = jnp.minimum(meta[:, CAP : CAP + 1], float(CAP))
    spots = spots.astype(jnp.int32)
    index = [spots[:, 8 * j : 8 * j + 8].reshape(-1) for j in range(8)]
    place = lax.broadcasted_iota(jnp.int32, (SIDE, 8), 1)
    index.append(jnp.where((8 * place + 8).astype(F32) < peers, 1, 8 - place).reshape(-1))
    middle = pl.pallas_call(
        middle_kernel,
        out_shape=buffer(pitch),
        in_specs=[IN_SMEM] * 9 + [IN_VMEM],
        out_specs=IN_VMEM,
        scratch_shapes=[vmem((2 * SUMS, SIDE), F32)] * 2,
        compiler_params=pltpu.CompilerParams(vmem_limit_bytes=16 * MIB),
        name="middle",
    )
    xb = vmem(((CAP + 1) * SIDE, SIDE), BF16)
    acc_x = vmem(((OWN + 1) * SIDE, SIDE), F32)
    acc = vmem(((CAP + 1) * SIDE, SIDE), F32)
    node = vmem((OWN * SIDE, SIDE), BF16)
    for iteration in range(ITERS):
        recv = swap(middle(*index, recv))
        last = iteration == ITERS - 1
        out = pl.pallas_call(
            functools.partial(tail_kernel, last, pitch),
            out_shape=(NODES, NODES) if last else buffer(pitch),
            in_specs=[IN_SMEM] + [IN_VMEM] * 4,
            out_specs=(IN_VMEM, IN_VMEM) if last else IN_VMEM,
            scratch_shapes=[wide(pitch), xb, acc_x, *(() if last else (acc, node, node))],
            compiler_params=pltpu.CompilerParams(vmem_limit_bytes=32 * MIB),
            name="last" if last else "tail",
        )(slots, recv, tile_values, source, target)
        if not last:
            recv = swap(out)
    return out


def general(source, target, tile_values, tile_rows, tile_peers, need_list, tile_count):
    peers_total = lax.axis_size("rows")
    row_count = source.shape[0] // SIDE
    tiles_here = tile_values.shape[0]
    group = min(16, tiles_here)
    live = (jnp.arange(tiles_here, dtype=jnp.int32) < tile_count[0]).astype(F32)[:, None, None]
    send_list = swap(need_list.reshape(peers_total, 1))[:, 0]
    owner_hot = (send_list[None, :] == jnp.arange(row_count, dtype=jnp.int32)[:, None]).astype(F32)

    def take(value, position):
        return lax.dynamic_slice_in_dim(value, position * group, group, 0)

    def product(form, vectors, position, ids):
        return (
            jnp.einsum(form, take(tile_values, position), vectors[ids], preferred_element_type=F32)
            * take(live, position)
        )

    def iterate(_, state):
        source_now, target_now = state
        source_blocks = source_now.reshape(row_count, SIDE, SIDE)
        target_blocks = target_now.reshape(row_count, SIDE, SIDE)

        def backward(position, running):
            part = product("tji,tjk->tik", target_blocks, position, take(tile_rows, position))
            return running.at[take(tile_peers, position)].add(part)

        partial = lax.fori_loop(
            0, tiles_here // group, backward, jnp.zeros((peers_total, SIDE, SIDE), F32)
        )
        both = swap(jnp.stack([source_blocks[send_list], partial.astype(BF16)], axis=1))
        fetched = both[:, 0]

        def forward(position, running):
            part = product("tij,tjk->tik", fetched, position, take(tile_peers, position))
            return running.at[take(tile_rows, position)].add(part)

        gathered = lax.fori_loop(
            0, tiles_here // group, forward, jnp.zeros((row_count, SIDE, SIDE), F32)
        )
        incoming = jnp.dot(
            owner_hot,
            both[:, 1].astype(F32).reshape(peers_total, -1),
            precision=lax.Precision.HIGHEST,
            preferred_element_type=F32,
        )
        return (
            settle(source, gathered.reshape(-1, SIDE)),
            settle(target, incoming.reshape(-1, SIDE)),
        )

    return lax.fori_loop(0, ITERS, iterate, (source, target))


def shards(*args):
    recv, meta, slots, nodes, which, most = begin(*args)
    onward = recv, meta, slots, *nodes, args[2]
    return lax.switch(
        which,
        [
            lambda: proceed(OWN + FEW, *onward),
            lambda: proceed(PITCH, *onward),
            lambda: general(*args[:6], jnp.where(most > 0, args[6], 0)),
        ],
    )


def solution(mesh):
    return jax.shard_map(
        shards,
        mesh=mesh,
        in_specs=(
            P("rows", None),
            P("rows", None),
            P("rows", None, None),
            P("rows"),
            P("rows"),
            P("rows", None),
            P("rows"),
        ),
        out_specs=(P("rows", None), P("rows", None)),
        check_vma=False,
    )
```

```python
import functools
import jax
import jax.numpy as jnp
from jax import lax
from jax.experimental import pallas as pl
from jax.experimental.pallas import tpu as pltpu
from jax.sharding import PartitionSpec as P

ITERS = 2
epsilon = 1e-06

SIDE = 128
OWN = 16
CAP = 63
FEW = 56
PITCH = OWN + CAP + 1
META = PITCH - 1
F32 = jnp.float32
BF16 = jnp.bfloat16
MIB = 1 << 20


def settle(base, update):
    total = base.astype(F32) + update
    scale = lax.rsqrt(jnp.mean(total * total, axis=-1, keepdims=True) + epsilon)
    return (total * scale).astype(BF16)


def block(ref, index):
    return ref[pl.ds(pl.multiple_of(index * SIDE, SIDE), SIDE), :]


def odd_pitch(pitch):
    return pitch + 1


def pack_rows(pitch, scr, x_ref, acc, peers, buf):
    stride = odd_pitch(pitch)
    for b in range(OWN):
        scr[pl.ds(b, SIDE, stride=stride), :] = x_ref[b * SIDE : (b + 1) * SIDE, :].astype(F32)

    def put(c, _):
        scr[pl.ds(OWN + c, SIDE, stride=stride), :] = block(acc, c)
        return 0

    lax.fori_loop(0, peers, put, 0)

    def narrow(i, _):
        buf[i] = scr[pl.ds(i * stride, pitch), :].astype(BF16)
        return 0

    lax.fori_loop(0, SIDE, narrow, 0, unroll=4)


def zero(ref, blocks):
    def one(c, _):
        ref[pl.ds(pl.multiple_of(c * SIDE, SIDE), SIDE), :] = jnp.zeros((SIDE, SIDE), F32)
        return 0

    lax.fori_loop(0, blocks, one, 0)


def back_dot(tile, y):
    return lax.dot_general(tile, y, (((0,), (0,)), ((), ())), preferred_element_type=F32)


STEP = 8
CHUNK = 16


def tile_copy(tiles, held, sems, c):
    at = pl.ds(pl.multiple_of(c * CHUNK, CHUNK), CHUNK)
    return pltpu.make_async_copy(tiles.at[at], held.at[at], sems.at[c])


def start_tiles(tiles, held, sems):
    for c in range(SIDE // CHUNK):
        tile_copy(tiles, held, sems, c).start()


def over_tiles(live, step, tiles=None, held=None, sems=None):
    if tiles is None:
        lax.fori_loop(0, (live + STEP - 1) // STEP, step, 0)
        return

    def chunk(c, _):
        tile_copy(tiles, held, sems, c).wait()
        first = c * (CHUNK // STEP)
        end = jnp.minimum((live + STEP - 1) // STEP, first + CHUNK // STEP)
        lax.fori_loop(first, end, step, 0)
        return 0

    lax.fori_loop(0, SIDE // CHUNK, chunk, 0)


def first_kernel(
    count, rows, peers_ref, need_ref, rows_ref, hbm, x_ref, y_ref, *rest
):
    buf, slots, x_kept, y_kept, scr, acc, slot_v, sem, tiles, sems = rest
    start_tiles(hbm, tiles, sems)
    x_kept[...] = x_ref[...]
    y_kept[...] = y_ref[...]
    live = count[0]
    row_at = lax.broadcasted_iota(jnp.int32, (SIDE, SIDE), 0)
    lane_at = lax.broadcasted_iota(jnp.int32, (SIDE, SIDE), 1)
    hit = jnp.where((row_at == peers_ref[...]) & (lane_at < live), 1.0, 0.0)
    used = jnp.broadcast_to(jnp.max(hit, axis=1, keepdims=True), (SIDE, SIDE))
    below = jnp.where(lane_at < row_at, 1.0, 0.0).astype(BF16)
    slot = jnp.dot(below, used.astype(BF16), preferred_element_type=F32)
    total = jnp.sum(used, axis=0, keepdims=True)
    lane = lax.broadcasted_iota(jnp.int32, (1, SIDE), 1)
    mine = jnp.sum(hit * slot, axis=0, keepdims=True)
    mine = jnp.where(lane < live, jnp.minimum(mine, float(CAP)), float(CAP))
    peer_total = jnp.minimum(total, float(CAP))
    slot_v[0:1, :] = mine.astype(jnp.int32)
    slot_v[1:2, :] = peer_total.astype(jnp.int32)
    slot_v[2:3, :] = rows_ref[...]
    slot_v[3:4, :] = jnp.zeros((1, SIDE), jnp.int32) + live
    copy = pltpu.make_async_copy(slot_v, slots, sem)
    copy.start()
    order = lane_at & CAP
    order = ((order & 7) * 8 + lax.shift_right_logical(order, 3)).astype(F32)
    pick = (used > 0) & (slot == order)
    peer_of = jnp.sum(jnp.where(pick, row_at.astype(F32), 0.0), axis=0, keepdims=True)
    peer_of = jnp.where(order[0:1, :] < total, peer_of, float(SIDE))
    need_col = jnp.sum(
        jnp.where(row_at == lane_at, need_ref[...], 0).astype(F32), axis=1, keepdims=True
    )
    need_of = jnp.sum(jnp.where(pick, need_col, 0.0), axis=0, keepdims=True)
    kind = jnp.where(total > FEW, 1.0, 0.0) + jnp.where(total > CAP, 1.0, 0.0)
    meta = jnp.where(lane < CAP, peer_of, jnp.where(lane == CAP, total, need_of))
    meta = jnp.where(lane == SIDE - 1, kind, meta)
    scr[pl.ds(META, SIDE, stride=odd_pitch(PITCH)), :] = jnp.broadcast_to(meta, (SIDE, SIDE))
    copy.wait()
    peers = slots[1, 0]
    zero(acc, peers)

    def step(g, _):
        parts = []
        for k in range(STEP):
            t = g * STEP + k
            parts.append((slots[0, t], back_dot(tiles[t], block(y_ref, rows[t]))))
        for s, part in parts:
            where = pl.ds(pl.multiple_of(s * SIDE, SIDE), SIDE)
            acc[where, :] = acc[where, :] + part
        return 0

    over_tiles(live, step, hbm, tiles, sems)
    pack_rows(PITCH, scr, x_ref, acc, peers, buf)


GROUPS = SIDE * (CAP + 1) // 8
PAD = 8
DUMMY = OWN * SIDE
SUMS = PAD + DUMMY + 16


def middle_kernel(*refs):
    *index, onward, recv, buf, even, odd = refs

    def load(d, _):
        at = pl.multiple_of(PAD + d * OWN, 8)
        rows = recv[d, 0:OWN, :].astype(F32)
        for ref in (even, odd):
            ref[pl.ds(at, OWN), :] = rows
            ref[pl.ds(SUMS + at, OWN), :] = jnp.zeros((OWN, SIDE), F32)
        return 0

    lax.fori_loop(0, SIDE, load, 0, unroll=4)
    row_at = lax.broadcasted_iota(jnp.int32, (8, SIDE), 0)

    def clip(group):
        return jnp.where(group < GROUPS, group, SIDE - 1)

    def work(groups):
        jobs = []
        for ref, group in zip((even, odd), groups):
            spots = [entry[clip(group)] for entry in index]
            start = OWN + lax.shift_right_logical(clip(group), 7) * 8
            at = clip(group) & (SIDE - 1), pl.ds(pl.multiple_of(start, 8), 8), slice(None)
            parts = jnp.where(group >= GROUPS, 0.0, recv[at].astype(F32))
            jobs.append((ref, spots, at, parts))
        found = []
        for ref, spots, at, parts in jobs:
            picked = ref[pl.ds(spots[0] + PAD, 8), :]
            sums = [ref[pl.ds(spots[0] + SUMS + PAD, 8), :] + parts]
            for j in range(1, 8):
                picked = jnp.where(row_at == j, ref[pl.ds(spots[j] + PAD - j, 8), :], picked)
                sums.append(ref[pl.ds(spots[j] + (SUMS + PAD - j), 8), :] + parts)
            found.append((picked, sums))
        for (ref, spots, at, _), (picked, sums) in zip(jobs, found):
            buf[at] = picked.astype(BF16)
            for j, spot in enumerate(spots):
                window = ref.at[pl.ds(spot + (SUMS + PAD - j), 8), :]
                pltpu.store(window, sums[j], mask=row_at == j)

    def two(groups):
        first = onward[groups[1]]
        second = onward[first]
        third = onward[second]
        fourth = onward[third]
        work(groups)
        work((first, second))
        return third, fourth

    lax.while_loop(lambda groups: groups[0] < GROUPS, two, (jnp.int32(0), onward[0]))

    def narrow(d, _):
        at = pl.ds(pl.multiple_of(SUMS + PAD + d * OWN, 8), OWN)
        buf[d, 0:OWN, :] = (even[at, :] + odd[at, :]).astype(BF16)
        return 0

    lax.fori_loop(0, SIDE, narrow, 0, unroll=4)


def tail_kernel(
    last, pitch, slots, recv, tiles, source, target, *rest
):
    if last:
        x_new, y_new, scr, xb, acc_x = rest
        buf = acc = None
    else:
        buf, scr, xb, acc_x, acc, x_new, y_new = rest
    live = slots[3, 0]
    peers = slots[1, 0]
    stride = odd_pitch(pitch)

    def widen(i, _):
        scr[pl.ds(i * stride, pitch), :] = recv[i].astype(F32)
        return 0

    lax.fori_loop(0, SIDE, widen, 0, unroll=4)
    for b in range(OWN):
        at = slice(b * SIDE, (b + 1) * SIDE)
        y_new[at, :] = settle(target[at, :], scr[pl.ds(b, SIDE, stride=stride), :])

    def fetch(c, _):
        xb[pl.ds(pl.multiple_of(c * SIDE, SIDE), SIDE), :] = scr[
            pl.ds(OWN + c, SIDE, stride=stride), :
        ].astype(BF16)
        return 0

    lax.fori_loop(0, peers, fetch, 0)
    zero(acc_x, OWN)
    if not last:
        zero(acc, peers)

    def step(g, _):
        ahead, back = [], []
        for k in range(STEP):
            t = g * STEP + k
            s, r, tile = slots[0, t], slots[2, t], tiles[t]
            to = jnp.where(t < live, r, OWN)
            ahead.append((to, jnp.dot(tile, block(xb, s), preferred_element_type=F32)))
            if not last:
                back.append((s, back_dot(tile, block(y_new, r))))
        for ref, found in ((acc_x, ahead), (acc, back)):
            for s, part in found:
                where = pl.ds(pl.multiple_of(s * SIDE, SIDE), SIDE)
                ref[where, :] = ref[where, :] + part
        return 0

    over_tiles(live, step)
    for b in range(OWN):
        at = slice(b * SIDE, (b + 1) * SIDE)
        x_new[at, :] = settle(source[at, :], acc_x[at, :])
    if not last:
        pack_rows(pitch, scr, x_new, acc, peers, buf)


def vmem(shape, dtype):
    return pltpu.VMEM(shape, dtype)


IN_VMEM = pl.BlockSpec(memory_space=pltpu.VMEM)
IN_SMEM = pl.BlockSpec(memory_space=pltpu.SMEM)
ANYWHERE = pl.BlockSpec(memory_space=pl.ANY)
NODES = jax.ShapeDtypeStruct((OWN * SIDE, SIDE), BF16)


def buffer(pitch):
    return jax.ShapeDtypeStruct((SIDE, pitch, SIDE), BF16)


def wide(pitch):
    return vmem((SIDE * odd_pitch(pitch), SIDE), F32)


def swap(value):
    return lax.all_to_all(value, "rows", split_axis=0, concat_axis=0, tiled=True)


def begin(source, target, tile_values, tile_rows, tile_peers, need_list, tile_count):
    buf, slots, *kept = pl.pallas_call(
        first_kernel,
        out_shape=(buffer(PITCH), jax.ShapeDtypeStruct((8, SIDE), jnp.int32), NODES, NODES),
        in_specs=[IN_SMEM] * 2 + [IN_VMEM] * 3 + [ANYWHERE] + [IN_VMEM] * 2,
        out_specs=(IN_VMEM, IN_SMEM, IN_VMEM, IN_VMEM),
        scratch_shapes=[
            wide(PITCH),
            vmem(((CAP + 1) * SIDE, SIDE), F32),
            vmem((8, SIDE), jnp.int32),
            pltpu.SemaphoreType.DMA,
            vmem((SIDE, SIDE, SIDE), BF16),
            pltpu.SemaphoreType.DMA((SIDE // CHUNK,)),
        ],
        compiler_params=pltpu.CompilerParams(vmem_limit_bytes=28 * MIB),
        name="first",
    )(
        tile_count,
        tile_rows,
        tile_peers.reshape(1, SIDE),
        need_list.reshape(1, SIDE),
        tile_rows.reshape(1, SIDE),
        tile_values,
        source,
        target,
    )
    recv = swap(buf)
    meta = recv[:, META, :].astype(F32)
    return recv, meta, slots, kept, jnp.max(meta[:, SIDE - 1].astype(jnp.int32))


def proceed(pitch, recv, meta, slots, source, target, tile_values):
    meta = meta.T
    row = lax.broadcasted_iota(jnp.int32, (CAP + 1, SIDE), 0)
    spots = meta[: CAP + 1] * OWN + meta[CAP + 1 :]
    spots = jnp.where(row == CAP, float(DUMMY), spots).astype(jnp.int32)
    peers = jnp.minimum(meta[CAP : CAP + 1], float(CAP))
    place, reader = row[:16], lax.broadcasted_iota(jnp.int32, (16, SIDE), 1)
    more = (8 * place + 8).astype(F32) < peers
    onward = jnp.where(reader == SIDE - 1, GROUPS, reader + 1)
    onward = jnp.where(more, (place + 1) * SIDE + reader, onward)
    onward = jnp.where(place >= 8, GROUPS, onward)
    index = [spots[8 * j : 8 * j + 8].reshape(-1) for j in range(8)] + [onward.reshape(-1)]
    middle = pl.pallas_call(
        middle_kernel,
        out_shape=buffer(pitch),
        in_specs=[IN_SMEM] * 9 + [IN_VMEM],
        out_specs=IN_VMEM,
        scratch_shapes=[vmem((2 * SUMS, SIDE), F32)] * 2,
        compiler_params=pltpu.CompilerParams(vmem_limit_bytes=16 * MIB),
        name="middle",
    )
    xb = vmem(((CAP + 1) * SIDE, SIDE), BF16)
    acc_x = vmem(((OWN + 1) * SIDE, SIDE), F32)
    acc = vmem(((CAP + 1) * SIDE, SIDE), F32)
    node = vmem((OWN * SIDE, SIDE), BF16)
    for iteration in range(ITERS):
        recv = swap(middle(*index, recv))
        last = iteration == ITERS - 1
        out = pl.pallas_call(
            functools.partial(tail_kernel, last, pitch),
            out_shape=(NODES, NODES) if last else buffer(pitch),
            in_specs=[IN_SMEM] + [IN_VMEM] * 4,
            out_specs=(IN_VMEM, IN_VMEM) if last else IN_VMEM,
            scratch_shapes=[wide(pitch), xb, acc_x, *(() if last else (acc, node, node))],
            compiler_params=pltpu.CompilerParams(vmem_limit_bytes=32 * MIB),
            name="last" if last else "tail",
        )(slots, recv, tile_values, source, target)
        if not last:
            recv = swap(out)
    return out


def general(source, target, tile_values, tile_rows, tile_peers, need_list, tile_count):
    peers_total = lax.axis_size("rows")
    row_count = source.shape[0] // SIDE
    tiles_here = tile_values.shape[0]
    group = min(16, tiles_here)
    live = (jnp.arange(tiles_here, dtype=jnp.int32) < tile_count[0]).astype(F32)[:, None, None]
    send_list = swap(need_list.reshape(peers_total, 1))[:, 0]
    owner_hot = (send_list[None, :] == jnp.arange(row_count, dtype=jnp.int32)[:, None]).astype(F32)

    def take(value, position):
        return lax.dynamic_slice_in_dim(value, position * group, group, 0)

    def product(form, vectors, position, ids):
        return (
            jnp.einsum(form, take(tile_values, position), vectors[ids], preferred_element_type=F32)
            * take(live, position)
        )

    def iterate(_, state):
        source_now, target_now = state
        source_blocks = source_now.reshape(row_count, SIDE, SIDE)
        target_blocks = target_now.reshape(row_count, SIDE, SIDE)

        def backward(position, running):
            part = product("tji,tjk->tik", target_blocks, position, take(tile_rows, position))
            return running.at[take(tile_peers, position)].add(part)

        partial = lax.fori_loop(
            0, tiles_here // group, backward, jnp.zeros((peers_total, SIDE, SIDE), F32)
        )
        both = swap(jnp.stack([source_blocks[send_list], partial.astype(BF16)], axis=1))
        fetched = both[:, 0]

        def forward(position, running):
            part = product("tij,tjk->tik", fetched, position, take(tile_peers, position))
            return running.at[take(tile_rows, position)].add(part)

        gathered = lax.fori_loop(
            0, tiles_here // group, forward, jnp.zeros((row_count, SIDE, SIDE), F32)
        )
        incoming = jnp.dot(
            owner_hot,
            both[:, 1].astype(F32).reshape(peers_total, -1),
            precision=lax.Precision.HIGHEST,
            preferred_element_type=F32,
        )
        return (
            settle(source, gathered.reshape(-1, SIDE)),
            settle(target, incoming.reshape(-1, SIDE)),
        )

    return lax.fori_loop(0, ITERS, iterate, (source, target))


def shards(*args):
    recv, meta, slots, nodes, which = begin(*args)
    onward = recv, meta, slots, *nodes, args[2]
    return lax.switch(
        which,
        [
            lambda: proceed(OWN + FEW, *onward),
            lambda: proceed(PITCH, *onward),
            lambda: general(*args[:6], jnp.where(which >= 0, args[6], 0)),
        ],
    )


def solution(mesh):
    return jax.shard_map(
        shards,
        mesh=mesh,
        in_specs=(
            P("rows", None),
            P("rows", None),
            P("rows", None, None),
            P("rows"),
            P("rows"),
            P("rows", None),
            P("rows"),
        ),
        out_specs=(P("rows", None), P("rows", None)),
        check_vma=False,
    )
```

```python
import functools
import jax
import jax.numpy as jnp
from jax import lax
from jax.experimental import pallas as pl
from jax.experimental.pallas import tpu as pltpu
from jax.sharding import PartitionSpec as P

ITERS = 2
epsilon = 1e-06

SIDE = 128
OWN = 16
CAP = 63
FEW = 56
PITCH = OWN + CAP + 1
META = PITCH - 1
F32 = jnp.float32
BF16 = jnp.bfloat16
MIB = 1 << 20


def settle(base, update):
    total = base.astype(F32) + update
    scale = lax.rsqrt(jnp.mean(total * total, axis=-1, keepdims=True) + epsilon)
    return (total * scale).astype(BF16)


def block(ref, index):
    return ref[pl.ds(pl.multiple_of(index * SIDE, SIDE), SIDE), :]


def odd_pitch(pitch):
    return pitch + 1


def pack_rows(pitch, scr, x_ref, acc, peers, buf):
    stride = odd_pitch(pitch)
    for b in range(OWN):
        scr[pl.ds(b, SIDE, stride=stride), :] = x_ref[b * SIDE : (b + 1) * SIDE, :].astype(F32)

    def put(c, _):
        scr[pl.ds(OWN + c, SIDE, stride=stride), :] = block(acc, c)
        return 0

    lax.fori_loop(0, peers, put, 0)

    def narrow(i, _):
        buf[i] = scr[pl.ds(i * stride, pitch), :].astype(BF16)
        return 0

    lax.fori_loop(0, SIDE, narrow, 0, unroll=4)


def zero(ref, blocks):
    def one(c, _):
        ref[pl.ds(pl.multiple_of(c * SIDE, SIDE), SIDE), :] = jnp.zeros((SIDE, SIDE), F32)
        return 0

    lax.fori_loop(0, blocks, one, 0)


def back_dot(tile, y):
    return lax.dot_general(tile, y, (((0,), (0,)), ((), ())), preferred_element_type=F32)


STEP = 32
CHUNK = 32


def tile_copy(tiles, held, sems, c):
    at = pl.ds(pl.multiple_of(c * CHUNK, CHUNK), CHUNK)
    return pltpu.make_async_copy(tiles.at[at], held.at[at], sems.at[c])


def start_tiles(tiles, held, sems):
    for c in range(SIDE // CHUNK):
        tile_copy(tiles, held, sems, c).start()


def over_tiles(live, step, tiles=None, held=None, sems=None):
    if tiles is None:
        lax.fori_loop(0, (live + STEP - 1) // STEP, step, 0)
        return

    def chunk(c, _):
        tile_copy(tiles, held, sems, c).wait()
        first = c * (CHUNK // STEP)
        end = jnp.minimum((live + STEP - 1) // STEP, first + CHUNK // STEP)
        lax.fori_loop(first, end, step, 0)
        return 0

    lax.fori_loop(0, SIDE // CHUNK, chunk, 0)


def first_kernel(
    count, rows, peers_ref, need_ref, rows_ref, hbm, x_ref, y_ref, *rest
):
    buf, slots, x_kept, y_kept, scr, acc, slot_v, sem, tiles, sems = rest
    start_tiles(hbm, tiles, sems)
    x_kept[...] = x_ref[...]
    y_kept[...] = y_ref[...]
    live = count[0]
    row_at = lax.broadcasted_iota(jnp.int32, (SIDE, SIDE), 0)
    lane_at = lax.broadcasted_iota(jnp.int32, (SIDE, SIDE), 1)
    hit = jnp.where((row_at == peers_ref[...]) & (lane_at < live), 1.0, 0.0)
    used = jnp.broadcast_to(jnp.max(hit, axis=1, keepdims=True), (SIDE, SIDE))
    below = jnp.where(lane_at < row_at, 1.0, 0.0).astype(BF16)
    slot = jnp.dot(below, used.astype(BF16), preferred_element_type=F32)
    total = jnp.sum(used, axis=0, keepdims=True)
    lane = lax.broadcasted_iota(jnp.int32, (1, SIDE), 1)
    mine = jnp.sum(hit * slot, axis=0, keepdims=True)
    mine = jnp.where(lane < live, jnp.minimum(mine, float(CAP)), float(CAP))
    peer_total = jnp.minimum(total, float(CAP))
    slot_v[0:1, :] = mine.astype(jnp.int32)
    slot_v[1:2, :] = peer_total.astype(jnp.int32)
    slot_v[2:3, :] = rows_ref[...]
    slot_v[3:4, :] = jnp.zeros((1, SIDE), jnp.int32) + live
    copy = pltpu.make_async_copy(slot_v, slots, sem)
    copy.start()
    order = lane_at & CAP
    order = ((order & 7) * 8 + lax.shift_right_logical(order, 3)).astype(F32)
    pick = (used > 0) & (slot == order)
    peer_of = jnp.sum(jnp.where(pick, row_at.astype(F32), 0.0), axis=0, keepdims=True)
    peer_of = jnp.where(order[0:1, :] < total, peer_of, float(SIDE))
    need_col = jnp.sum(
        jnp.where(row_at == lane_at, need_ref[...], 0).astype(F32), axis=1, keepdims=True
    )
    need_of = jnp.sum(jnp.where(pick, need_col, 0.0), axis=0, keepdims=True)
    kind = jnp.where(total > FEW, 1.0, 0.0) + jnp.where(total > CAP, 1.0, 0.0)
    meta = jnp.where(lane < CAP, peer_of, jnp.where(lane == CAP, total, need_of))
    meta = jnp.where(lane == SIDE - 1, kind, meta)
    scr[pl.ds(META, SIDE, stride=odd_pitch(PITCH)), :] = jnp.broadcast_to(meta, (SIDE, SIDE))
    copy.wait()
    peers = slots[1, 0]
    zero(acc, peers)

    def step(g, _):
        parts = []
        for k in range(STEP):
            t = g * STEP + k
            parts.append((slots[0, t], back_dot(tiles[t], block(y_ref, rows[t]))))
        for s, part in parts:
            where = pl.ds(pl.multiple_of(s * SIDE, SIDE), SIDE)
            acc[where, :] = acc[where, :] + part
        return 0

    over_tiles(live, step, hbm, tiles, sems)
    pack_rows(PITCH, scr, x_ref, acc, peers, buf)


GROUPS = SIDE * (CAP + 1) // 8
PAD = 8
DUMMY = OWN * SIDE
SUMS = PAD + DUMMY + 16


def middle_kernel(*refs):
    *index, onward, recv, buf, even, odd = refs

    def load(d, _):
        at = pl.multiple_of(PAD + d * OWN, 8)
        rows = recv[d, 0:OWN, :].astype(F32)
        for ref in (even, odd):
            ref[pl.ds(at, OWN), :] = rows
            ref[pl.ds(SUMS + at, OWN), :] = jnp.zeros((OWN, SIDE), F32)
        return 0

    lax.fori_loop(0, SIDE, load, 0, unroll=4)
    row_at = lax.broadcasted_iota(jnp.int32, (8, SIDE), 0)

    def clip(group):
        return jnp.where(group < GROUPS, group, SIDE - 1)

    def work(groups):
        jobs = []
        for ref, group in zip((even, odd), groups):
            spots = [entry[clip(group)] for entry in index]
            start = OWN + lax.shift_right_logical(clip(group), 7) * 8
            at = clip(group) & (SIDE - 1), pl.ds(pl.multiple_of(start, 8), 8), slice(None)
            parts = jnp.where(group >= GROUPS, 0.0, recv[at].astype(F32))
            jobs.append((ref, spots, at, parts))
        found = []
        for ref, spots, at, parts in jobs:
            picked = ref[pl.ds(spots[0] + PAD, 8), :]
            sums = [ref[pl.ds(spots[0] + SUMS + PAD, 8), :] + parts]
            for j in range(1, 8):
                picked = jnp.where(row_at == j, ref[pl.ds(spots[j] + PAD - j, 8), :], picked)
                sums.append(ref[pl.ds(spots[j] + (SUMS + PAD - j), 8), :] + parts)
            found.append((picked, sums))
        for (ref, spots, at, _), (picked, sums) in zip(jobs, found):
            buf[at] = picked.astype(BF16)
            for j, spot in enumerate(spots):
                window = ref.at[pl.ds(spot + (SUMS + PAD - j), 8), :]
                pltpu.store(window, sums[j], mask=row_at == j)

    def two(groups):
        first = onward[groups[1]]
        second = onward[first]
        third = onward[second]
        fourth = onward[third]
        work(groups)
        work((first, second))
        return third, fourth

    lax.while_loop(lambda groups: groups[0] < GROUPS, two, (jnp.int32(0), onward[0]))

    def narrow(d, _):
        at = pl.ds(pl.multiple_of(SUMS + PAD + d * OWN, 8), OWN)
        buf[d, 0:OWN, :] = (even[at, :] + odd[at, :]).astype(BF16)
        return 0

    lax.fori_loop(0, SIDE, narrow, 0, unroll=4)


def tail_kernel(
    last, pitch, slots, recv, tiles, source, target, *rest
):
    if last:
        x_new, y_new, scr, xb, acc_x = rest
        buf = acc = None
    else:
        buf, scr, xb, acc_x, acc, x_new, y_new = rest
    live = slots[3, 0]
    peers = slots[1, 0]
    stride = odd_pitch(pitch)

    def widen(i, _):
        scr[pl.ds(i * stride, pitch), :] = recv[i].astype(F32)
        return 0

    lax.fori_loop(0, SIDE, widen, 0, unroll=4)
    for b in range(OWN):
        at = slice(b * SIDE, (b + 1) * SIDE)
        y_new[at, :] = settle(target[at, :], scr[pl.ds(b, SIDE, stride=stride), :])

    def fetch(c, _):
        xb[pl.ds(pl.multiple_of(c * SIDE, SIDE), SIDE), :] = scr[
            pl.ds(OWN + c, SIDE, stride=stride), :
        ].astype(BF16)
        return 0

    lax.fori_loop(0, peers, fetch, 0)
    zero(acc_x, OWN)
    if not last:
        zero(acc, peers)

    def step(g, _):
        ahead, back = [], []
        for k in range(STEP):
            t = g * STEP + k
            s, r, tile = slots[0, t], slots[2, t], tiles[t]
            to = jnp.where(t < live, r, OWN)
            ahead.append((to, jnp.dot(tile, block(xb, s), preferred_element_type=F32)))
            if not last:
                back.append((s, back_dot(tile, block(y_new, r))))
        for ref, found in ((acc_x, ahead), (acc, back)):
            for s, part in found:
                where = pl.ds(pl.multiple_of(s * SIDE, SIDE), SIDE)
                ref[where, :] = ref[where, :] + part
        return 0

    over_tiles(live, step)
    for b in range(OWN):
        at = slice(b * SIDE, (b + 1) * SIDE)
        x_new[at, :] = settle(source[at, :], acc_x[at, :])
    if not last:
        pack_rows(pitch, scr, x_new, acc, peers, buf)


def vmem(shape, dtype):
    return pltpu.VMEM(shape, dtype)


IN_VMEM = pl.BlockSpec(memory_space=pltpu.VMEM)
IN_SMEM = pl.BlockSpec(memory_space=pltpu.SMEM)
ANYWHERE = pl.BlockSpec(memory_space=pl.ANY)
NODES = jax.ShapeDtypeStruct((OWN * SIDE, SIDE), BF16)


def buffer(pitch):
    return jax.ShapeDtypeStruct((SIDE, pitch, SIDE), BF16)


def wide(pitch):
    return vmem((SIDE * odd_pitch(pitch), SIDE), F32)


def swap(value):
    return lax.all_to_all(value, "rows", split_axis=0, concat_axis=0, tiled=True)


def begin(source, target, tile_values, tile_rows, tile_peers, need_list, tile_count):
    buf, slots, *kept = pl.pallas_call(
        first_kernel,
        out_shape=(buffer(PITCH), jax.ShapeDtypeStruct((8, SIDE), jnp.int32), NODES, NODES),
        in_specs=[IN_SMEM] * 2 + [IN_VMEM] * 3 + [ANYWHERE] + [IN_VMEM] * 2,
        out_specs=(IN_VMEM, IN_SMEM, IN_VMEM, IN_VMEM),
        scratch_shapes=[
            wide(PITCH),
            vmem(((CAP + 1) * SIDE, SIDE), F32),
            vmem((8, SIDE), jnp.int32),
            pltpu.SemaphoreType.DMA,
            vmem((SIDE, SIDE, SIDE), BF16),
            pltpu.SemaphoreType.DMA((SIDE // CHUNK,)),
        ],
        compiler_params=pltpu.CompilerParams(vmem_limit_bytes=28 * MIB),
        name="first",
    )(
        tile_count,
        tile_rows,
        tile_peers.reshape(1, SIDE),
        need_list.reshape(1, SIDE),
        tile_rows.reshape(1, SIDE),
        tile_values,
        source,
        target,
    )
    recv = swap(buf)
    meta = recv[:, META, :].astype(F32)
    return recv, meta, slots, kept, jnp.max(meta[:, SIDE - 1].astype(jnp.int32))


def proceed(pitch, recv, meta, slots, source, target, tile_values):
    meta = meta.T
    row = lax.broadcasted_iota(jnp.int32, (CAP + 1, SIDE), 0)
    spots = meta[: CAP + 1] * OWN + meta[CAP + 1 :]
    spots = jnp.where(row == CAP, float(DUMMY), spots).astype(jnp.int32)
    peers = jnp.minimum(meta[CAP : CAP + 1], float(CAP))
    place, reader = row[:16], lax.broadcasted_iota(jnp.int32, (16, SIDE), 1)
    more = (8 * place + 8).astype(F32) < peers
    onward = jnp.where(reader == SIDE - 1, GROUPS, reader + 1)
    onward = jnp.where(more, (place + 1) * SIDE + reader, onward)
    onward = jnp.where(place >= 8, GROUPS, onward)
    index = [spots[8 * j : 8 * j + 8].reshape(-1) for j in range(8)] + [onward.reshape(-1)]
    middle = pl.pallas_call(
        middle_kernel,
        out_shape=buffer(pitch),
        in_specs=[IN_SMEM] * 9 + [IN_VMEM],
        out_specs=IN_VMEM,
        scratch_shapes=[vmem((2 * SUMS, SIDE), F32)] * 2,
        compiler_params=pltpu.CompilerParams(vmem_limit_bytes=16 * MIB),
        name="middle",
    )
    xb = vmem(((CAP + 1) * SIDE, SIDE), BF16)
    acc_x = vmem(((OWN + 1) * SIDE, SIDE), F32)
    acc = vmem(((CAP + 1) * SIDE, SIDE), F32)
    node = vmem((OWN * SIDE, SIDE), BF16)
    for iteration in range(ITERS):
        recv = swap(middle(*index, recv))
        last = iteration == ITERS - 1
        out = pl.pallas_call(
            functools.partial(tail_kernel, last, pitch),
            out_shape=(NODES, NODES) if last else buffer(pitch),
            in_specs=[IN_SMEM] + [IN_VMEM] * 4,
            out_specs=(IN_VMEM, IN_VMEM) if last else IN_VMEM,
            scratch_shapes=[wide(pitch), xb, acc_x, *(() if last else (acc, node, node))],
            compiler_params=pltpu.CompilerParams(vmem_limit_bytes=32 * MIB),
            name="last" if last else "tail",
        )(slots, recv, tile_values, source, target)
        if not last:
            recv = swap(out)
    return out


def general(source, target, tile_values, tile_rows, tile_peers, need_list, tile_count):
    peers_total = lax.axis_size("rows")
    row_count = source.shape[0] // SIDE
    tiles_here = tile_values.shape[0]
    group = min(16, tiles_here)
    live = (jnp.arange(tiles_here, dtype=jnp.int32) < tile_count[0]).astype(F32)[:, None, None]
    send_list = swap(need_list.reshape(peers_total, 1))[:, 0]
    owner_hot = (send_list[None, :] == jnp.arange(row_count, dtype=jnp.int32)[:, None]).astype(F32)

    def take(value, position):
        return lax.dynamic_slice_in_dim(value, position * group, group, 0)

    def product(form, vectors, position, ids):
        return (
            jnp.einsum(form, take(tile_values, position), vectors[ids], preferred_element_type=F32)
            * take(live, position)
        )

    def iterate(_, state):
        source_now, target_now = state
        source_blocks = source_now.reshape(row_count, SIDE, SIDE)
        target_blocks = target_now.reshape(row_count, SIDE, SIDE)

        def backward(position, running):
            part = product("tji,tjk->tik", target_blocks, position, take(tile_rows, position))
            return running.at[take(tile_peers, position)].add(part)

        partial = lax.fori_loop(
            0, tiles_here // group, backward, jnp.zeros((peers_total, SIDE, SIDE), F32)
        )
        both = swap(jnp.stack([source_blocks[send_list], partial.astype(BF16)], axis=1))
        fetched = both[:, 0]

        def forward(position, running):
            part = product("tij,tjk->tik", fetched, position, take(tile_peers, position))
            return running.at[take(tile_rows, position)].add(part)

        gathered = lax.fori_loop(
            0, tiles_here // group, forward, jnp.zeros((row_count, SIDE, SIDE), F32)
        )
        incoming = jnp.dot(
            owner_hot,
            both[:, 1].astype(F32).reshape(peers_total, -1),
            precision=lax.Precision.HIGHEST,
            preferred_element_type=F32,
        )
        return (
            settle(source, gathered.reshape(-1, SIDE)),
            settle(target, incoming.reshape(-1, SIDE)),
        )

    return lax.fori_loop(0, ITERS, iterate, (source, target))


def shards(*args):
    recv, meta, slots, nodes, which = begin(*args)
    onward = recv, meta, slots, *nodes, args[2]
    return lax.switch(
        which,
        [
            lambda: proceed(OWN + FEW, *onward),
            lambda: proceed(PITCH, *onward),
            lambda: general(*args[:6], jnp.where(which >= 0, args[6], 0)),
        ],
    )


def solution(mesh):
    return jax.shard_map(
        shards,
        mesh=mesh,
        in_specs=(
            P("rows", None),
            P("rows", None),
            P("rows", None, None),
            P("rows"),
            P("rows"),
            P("rows", None),
            P("rows"),
        ),
        out_specs=(P("rows", None), P("rows", None)),
        check_vma=False,
    )
```

```python
import functools
import jax
import jax.numpy as jnp
from jax import lax
from jax.experimental import pallas as pl
from jax.experimental.pallas import tpu as pltpu
from jax.sharding import PartitionSpec as P

ITERS = 2
epsilon = 1e-06

SIDE = 128
OWN = 16
CAP = 63
FEW = 56
PITCH = OWN + CAP + 1
META = PITCH - 1
F32 = jnp.float32
BF16 = jnp.bfloat16
MIB = 1 << 20


def settle(base, update):
    total = base.astype(F32) + update
    scale = lax.rsqrt(jnp.mean(total * total, axis=-1, keepdims=True) + epsilon)
    return (total * scale).astype(BF16)


def block(ref, index):
    return ref[pl.ds(pl.multiple_of(index * SIDE, SIDE), SIDE), :]


def odd_pitch(pitch):
    return pitch + 1


def pack_rows(pitch, scr, x_ref, acc, peers, buf):
    stride = odd_pitch(pitch)
    for b in range(OWN):
        scr[pl.ds(b, SIDE, stride=stride), :] = x_ref[b * SIDE : (b + 1) * SIDE, :].astype(F32)

    def put(c, _):
        scr[pl.ds(OWN + c, SIDE, stride=stride), :] = block(acc, c)
        return 0

    lax.fori_loop(0, peers, put, 0)

    def narrow(i, _):
        buf[i] = scr[pl.ds(i * stride, pitch), :].astype(BF16)
        return 0

    lax.fori_loop(0, SIDE, narrow, 0, unroll=4)


def zero(ref, blocks):
    def one(c, _):
        ref[pl.ds(pl.multiple_of(c * SIDE, SIDE), SIDE), :] = jnp.zeros((SIDE, SIDE), F32)
        return 0

    lax.fori_loop(0, blocks, one, 0)


def back_dot(tile, y):
    return lax.dot_general(tile, y, (((0,), (0,)), ((), ())), preferred_element_type=F32)


STEP = 32
CHUNK = 32


def tile_copy(tiles, held, sems, c):
    at = pl.ds(pl.multiple_of(c * CHUNK, CHUNK), CHUNK)
    return pltpu.make_async_copy(tiles.at[at], held.at[at], sems.at[c])


def start_tiles(tiles, held, sems):
    for c in range(SIDE // CHUNK):
        tile_copy(tiles, held, sems, c).start()


def over_tiles(live, step, tiles=None, held=None, sems=None):
    if tiles is None:
        lax.fori_loop(0, (live + STEP - 1) // STEP, step, 0)
        return

    def chunk(c, _):
        tile_copy(tiles, held, sems, c).wait()
        first = c * (CHUNK // STEP)
        end = jnp.minimum((live + STEP - 1) // STEP, first + CHUNK // STEP)
        lax.fori_loop(first, end, step, 0)
        return 0

    lax.fori_loop(0, SIDE // CHUNK, chunk, 0)


def first_kernel(
    count, rows, peers_ref, need_ref, rows_ref, hbm, x_ref, y_ref, *rest
):
    buf, slots, x_kept, y_kept, scr, acc, slot_v, sem, tiles, sems = rest
    start_tiles(hbm, tiles, sems)
    x_kept[...] = x_ref[...]
    y_kept[...] = y_ref[...]
    live = count[0]
    row_at = lax.broadcasted_iota(jnp.int32, (SIDE, SIDE), 0)
    lane_at = lax.broadcasted_iota(jnp.int32, (SIDE, SIDE), 1)
    hit = jnp.where((row_at == peers_ref[...]) & (lane_at < live), 1.0, 0.0)
    used = jnp.broadcast_to(jnp.max(hit, axis=1, keepdims=True), (SIDE, SIDE))
    below = jnp.where(lane_at < row_at, 1.0, 0.0).astype(BF16)
    slot = jnp.dot(below, used.astype(BF16), preferred_element_type=F32)
    total = jnp.sum(used, axis=0, keepdims=True)
    lane = lax.broadcasted_iota(jnp.int32, (1, SIDE), 1)
    mine = jnp.sum(hit * slot, axis=0, keepdims=True)
    mine = jnp.where(lane < live, jnp.minimum(mine, float(CAP)), float(CAP))
    peer_total = jnp.minimum(total, float(CAP))
    slot_v[0:1, :] = mine.astype(jnp.int32)
    slot_v[1:2, :] = peer_total.astype(jnp.int32)
    slot_v[2:3, :] = rows_ref[...]
    slot_v[3:4, :] = jnp.zeros((1, SIDE), jnp.int32) + live
    copy = pltpu.make_async_copy(slot_v, slots, sem)
    copy.start()
    order = lane_at & CAP
    order = ((order & 7) * 8 + lax.shift_right_logical(order, 3)).astype(F32)
    pick = (used > 0) & (slot == order)
    peer_of = jnp.sum(jnp.where(pick, row_at.astype(F32), 0.0), axis=0, keepdims=True)
    peer_of = jnp.where(order[0:1, :] < total, peer_of, float(SIDE))
    need_col = jnp.sum(
        jnp.where(row_at == lane_at, need_ref[...], 0).astype(F32), axis=1, keepdims=True
    )
    need_of = jnp.sum(jnp.where(pick, need_col, 0.0), axis=0, keepdims=True)
    kind = jnp.where(total > FEW, 1.0, 0.0) + jnp.where(total > CAP, 1.0, 0.0)
    meta = jnp.where(lane < CAP, peer_of, jnp.where(lane == CAP, total, need_of))
    meta = jnp.where(lane == SIDE - 1, kind, meta)
    scr[pl.ds(META, SIDE, stride=odd_pitch(PITCH)), :] = jnp.broadcast_to(meta, (SIDE, SIDE))
    copy.wait()
    peers = slots[1, 0]
    zero(acc, peers)

    def step(g, _):
        parts = []
        for k in range(STEP):
            t = g * STEP + k
            parts.append((slots[0, t], back_dot(tiles[t], block(y_ref, rows[t]))))
        for s, part in parts:
            where = pl.ds(pl.multiple_of(s * SIDE, SIDE), SIDE)
            acc[where, :] = acc[where, :] + part
        return 0

    over_tiles(live, step, hbm, tiles, sems)
    pack_rows(PITCH, scr, x_ref, acc, peers, buf)


GROUPS = SIDE * (CAP + 1) // 8
PAD = 8
DUMMY = OWN * SIDE
SUMS = PAD + DUMMY + 16


def middle_kernel(*refs):
    *index, onward, recv, buf, even, odd = refs

    def load(d, _):
        at = pl.multiple_of(PAD + d * OWN, 8)
        rows = recv[d, 0:OWN, :].astype(F32)
        for ref in (even, odd):
            ref[pl.ds(at, OWN), :] = rows
            ref[pl.ds(SUMS + at, OWN), :] = jnp.zeros((OWN, SIDE), F32)
        return 0

    lax.fori_loop(0, SIDE, load, 0, unroll=4)
    row_at = lax.broadcasted_iota(jnp.int32, (8, SIDE), 0)

    def clip(group):
        return jnp.where(group < GROUPS, group, SIDE - 1)

    def work(groups):
        jobs = []
        for ref, group in zip((even, odd), groups):
            spots = [entry[clip(group)] for entry in index]
            start = OWN + lax.shift_right_logical(clip(group), 7) * 8
            at = clip(group) & (SIDE - 1), pl.ds(pl.multiple_of(start, 8), 8), slice(None)
            parts = jnp.where(group >= GROUPS, 0.0, recv[at].astype(F32))
            jobs.append((ref, spots, at, parts))
        found = []
        for ref, spots, at, parts in jobs:
            picked = ref[pl.ds(spots[0] + PAD, 8), :]
            sums = [ref[pl.ds(spots[0] + SUMS + PAD, 8), :] + parts]
            for j in range(1, 8):
                picked = jnp.where(row_at == j, ref[pl.ds(spots[j] + PAD - j, 8), :], picked)
                sums.append(ref[pl.ds(spots[j] + (SUMS + PAD - j), 8), :] + parts)
            found.append((picked, sums))
        for (ref, spots, at, _), (picked, sums) in zip(jobs, found):
            buf[at] = picked.astype(BF16)
            for j, spot in enumerate(spots):
                window = ref.at[pl.ds(spot + (SUMS + PAD - j), 8), :]
                pltpu.store(window, sums[j], mask=row_at == j)

    def several(groups):
        for _ in range(4):
            first = onward[groups[1]]
            later = first, onward[first]
            work(groups)
            groups = later
        return groups

    lax.while_loop(lambda groups: groups[0] < GROUPS, several, (jnp.int32(0), onward[0]))

    def narrow(d, _):
        at = pl.ds(pl.multiple_of(SUMS + PAD + d * OWN, 8), OWN)
        buf[d, 0:OWN, :] = (even[at, :] + odd[at, :]).astype(BF16)
        return 0

    lax.fori_loop(0, SIDE, narrow, 0, unroll=4)


def tail_kernel(
    last, pitch, slots, recv, tiles, source, target, *rest
):
    if last:
        x_new, y_new, scr, xb, acc_x = rest
        buf = acc = None
    else:
        buf, scr, xb, acc_x, acc, x_new, y_new = rest
    live = slots[3, 0]
    peers = slots[1, 0]
    stride = odd_pitch(pitch)

    def widen(i, _):
        scr[pl.ds(i * stride, pitch), :] = recv[i].astype(F32)
        return 0

    lax.fori_loop(0, SIDE, widen, 0, unroll=4)
    for b in range(OWN):
        at = slice(b * SIDE, (b + 1) * SIDE)
        y_new[at, :] = settle(target[at, :], scr[pl.ds(b, SIDE, stride=stride), :])

    def fetch(c, _):
        xb[pl.ds(pl.multiple_of(c * SIDE, SIDE), SIDE), :] = scr[
            pl.ds(OWN + c, SIDE, stride=stride), :
        ].astype(BF16)
        return 0

    lax.fori_loop(0, peers, fetch, 0)
    zero(acc_x, OWN)
    if not last:
        zero(acc, peers)

    def step(g, _):
        ahead, back = [], []
        for k in range(STEP):
            t = g * STEP + k
            s, r, tile = slots[0, t], slots[2, t], tiles[t]
            to = jnp.where(t < live, r, OWN)
            ahead.append((to, jnp.dot(tile, block(xb, s), preferred_element_type=F32)))
            if not last:
                back.append((s, back_dot(tile, block(y_new, r))))
        for ref, found in ((acc_x, ahead), (acc, back)):
            for s, part in found:
                where = pl.ds(pl.multiple_of(s * SIDE, SIDE), SIDE)
                ref[where, :] = ref[where, :] + part
        return 0

    over_tiles(live, step)
    for b in range(OWN):
        at = slice(b * SIDE, (b + 1) * SIDE)
        x_new[at, :] = settle(source[at, :], acc_x[at, :])
    if not last:
        pack_rows(pitch, scr, x_new, acc, peers, buf)


def vmem(shape, dtype):
    return pltpu.VMEM(shape, dtype)


IN_VMEM = pl.BlockSpec(memory_space=pltpu.VMEM)
IN_SMEM = pl.BlockSpec(memory_space=pltpu.SMEM)
ANYWHERE = pl.BlockSpec(memory_space=pl.ANY)
NODES = jax.ShapeDtypeStruct((OWN * SIDE, SIDE), BF16)


def buffer(pitch):
    return jax.ShapeDtypeStruct((SIDE, pitch, SIDE), BF16)


def wide(pitch):
    return vmem((SIDE * odd_pitch(pitch), SIDE), F32)


def swap(value):
    return lax.all_to_all(value, "rows", split_axis=0, concat_axis=0, tiled=True)


def begin(source, target, tile_values, tile_rows, tile_peers, need_list, tile_count):
    buf, slots, *kept = pl.pallas_call(
        first_kernel,
        out_shape=(buffer(PITCH), jax.ShapeDtypeStruct((8, SIDE), jnp.int32), NODES, NODES),
        in_specs=[IN_SMEM] * 2 + [IN_VMEM] * 3 + [ANYWHERE] + [IN_VMEM] * 2,
        out_specs=(IN_VMEM, IN_SMEM, IN_VMEM, IN_VMEM),
        scratch_shapes=[
            wide(PITCH),
            vmem(((CAP + 1) * SIDE, SIDE), F32),
            vmem((8, SIDE), jnp.int32),
            pltpu.SemaphoreType.DMA,
            vmem((SIDE, SIDE, SIDE), BF16),
            pltpu.SemaphoreType.DMA((SIDE // CHUNK,)),
        ],
        compiler_params=pltpu.CompilerParams(vmem_limit_bytes=28 * MIB),
        name="first",
    )(
        tile_count,
        tile_rows,
        tile_peers.reshape(1, SIDE),
        need_list.reshape(1, SIDE),
        tile_rows.reshape(1, SIDE),
        tile_values,
        source,
        target,
    )
    recv = swap(buf)
    meta = recv[:, META, :].astype(F32)
    return recv, meta, slots, kept, jnp.max(meta[:, SIDE - 1].astype(jnp.int32))


def proceed(pitch, recv, meta, slots, source, target, tile_values):
    meta = meta.T
    row = lax.broadcasted_iota(jnp.int32, (CAP + 1, SIDE), 0)
    spots = meta[: CAP + 1] * OWN + meta[CAP + 1 :]
    spots = jnp.where(row == CAP, float(DUMMY), spots).astype(jnp.int32)
    peers = jnp.minimum(meta[CAP : CAP + 1], float(CAP))
    place, reader = row[:16], lax.broadcasted_iota(jnp.int32, (16, SIDE), 1)
    more = (8 * place + 8).astype(F32) < peers
    onward = jnp.where(reader == SIDE - 1, GROUPS, reader + 1)
    onward = jnp.where(more, (place + 1) * SIDE + reader, onward)
    onward = jnp.where(place >= 8, GROUPS, onward)
    index = [spots[8 * j : 8 * j + 8].reshape(-1) for j in range(8)] + [onward.reshape(-1)]
    middle = pl.pallas_call(
        middle_kernel,
        out_shape=buffer(pitch),
        in_specs=[IN_SMEM] * 9 + [IN_VMEM],
        out_specs=IN_VMEM,
        scratch_shapes=[vmem((2 * SUMS, SIDE), F32)] * 2,
        compiler_params=pltpu.CompilerParams(vmem_limit_bytes=16 * MIB),
        name="middle",
    )
    xb = vmem(((CAP + 1) * SIDE, SIDE), BF16)
    acc_x = vmem(((OWN + 1) * SIDE, SIDE), F32)
    acc = vmem(((CAP + 1) * SIDE, SIDE), F32)
    node = vmem((OWN * SIDE, SIDE), BF16)
    for iteration in range(ITERS):
        recv = swap(middle(*index, recv))
        last = iteration == ITERS - 1
        out = pl.pallas_call(
            functools.partial(tail_kernel, last, pitch),
            out_shape=(NODES, NODES) if last else buffer(pitch),
            in_specs=[IN_SMEM] + [IN_VMEM] * 4,
            out_specs=(IN_VMEM, IN_VMEM) if last else IN_VMEM,
            scratch_shapes=[wide(pitch), xb, acc_x, *(() if last else (acc, node, node))],
            compiler_params=pltpu.CompilerParams(vmem_limit_bytes=32 * MIB),
            name="last" if last else "tail",
        )(slots, recv, tile_values, source, target)
        if not last:
            recv = swap(out)
    return out


def general(source, target, tile_values, tile_rows, tile_peers, need_list, tile_count):
    peers_total = lax.axis_size("rows")
    row_count = source.shape[0] // SIDE
    tiles_here = tile_values.shape[0]
    group = min(16, tiles_here)
    live = (jnp.arange(tiles_here, dtype=jnp.int32) < tile_count[0]).astype(F32)[:, None, None]
    send_list = swap(need_list.reshape(peers_total, 1))[:, 0]
    owner_hot = (send_list[None, :] == jnp.arange(row_count, dtype=jnp.int32)[:, None]).astype(F32)

    def take(value, position):
        return lax.dynamic_slice_in_dim(value, position * group, group, 0)

    def product(form, vectors, position, ids):
        return (
            jnp.einsum(form, take(tile_values, position), vectors[ids], preferred_element_type=F32)
            * take(live, position)
        )

    def iterate(_, state):
        source_now, target_now = state
        source_blocks = source_now.reshape(row_count, SIDE, SIDE)
        target_blocks = target_now.reshape(row_count, SIDE, SIDE)

        def backward(position, running):
            part = product("tji,tjk->tik", target_blocks, position, take(tile_rows, position))
            return running.at[take(tile_peers, position)].add(part)

        partial = lax.fori_loop(
            0, tiles_here // group, backward, jnp.zeros((peers_total, SIDE, SIDE), F32)
        )
        both = swap(jnp.stack([source_blocks[send_list], partial.astype(BF16)], axis=1))
        fetched = both[:, 0]

        def forward(position, running):
            part = product("tij,tjk->tik", fetched, position, take(tile_peers, position))
            return running.at[take(tile_rows, position)].add(part)

        gathered = lax.fori_loop(
            0, tiles_here // group, forward, jnp.zeros((row_count, SIDE, SIDE), F32)
        )
        incoming = jnp.dot(
            owner_hot,
            both[:, 1].astype(F32).reshape(peers_total, -1),
            precision=lax.Precision.HIGHEST,
            preferred_element_type=F32,
        )
        return (
            settle(source, gathered.reshape(-1, SIDE)),
            settle(target, incoming.reshape(-1, SIDE)),
        )

    return lax.fori_loop(0, ITERS, iterate, (source, target))


def shards(*args):
    recv, meta, slots, nodes, which = begin(*args)
    onward = recv, meta, slots, *nodes, args[2]
    return lax.switch(
        which,
        [
            lambda: proceed(OWN + FEW, *onward),
            lambda: proceed(PITCH, *onward),
            lambda: general(*args[:6], jnp.where(which >= 0, args[6], 0)),
        ],
    )


def solution(mesh):
    return jax.shard_map(
        shards,
        mesh=mesh,
        in_specs=(
            P("rows", None),
            P("rows", None),
            P("rows", None, None),
            P("rows"),
            P("rows"),
            P("rows", None),
            P("rows"),
        ),
        out_specs=(P("rows", None), P("rows", None)),
        check_vma=False,
    )
```
